256 devices in a mesh: gz: 32 (over x, z), gy: 8 (over y, core).
Axes of the slice: x: 4, y: 4, z: 8, core: 2. Of those that a mesh axis runs over, the one named last changes fastest.
Arguments:
- ranks: float32 [256, 128, 512], P('gz', 'gy'), may hold values from 1 to 2
- seeds: float32 [3, 256, 128, 512], P(None, 'gz', 'gy'), may hold values from 0.25 to 1
- flags: int32 [256, 128, 512], P('gz', 'gy'), may hold values 0 or 1
Outputs:
- states: int32 [256, 128, 512], P('gz', 'gy')
- undecided: int32 [3], replicated
The draws below stay inside these ranges and needn't reach their ends.
All inputs are finite; a program needn't handle non-finite values. No bound on the sum of `flags` on one device may be relied on, other than what follows from the above.
Results may differ from the reference program's by a relative error of at most 0.000001.
Values sent between devices are 32-bit elements; how exact they have to be, the bound alone decides.
A program may use at most 64 MiB of HBM per device.

```python
import math
import jax
import jax.numpy as jnp

NX = 512
ROUNDS = 3
NY = 128
NZ = 256


def set_ends(drawn, key, low, top_value):
    extent = drawn.shape
    spot = [jax.random.randint(jax.random.fold_in(key, axis), (), 0, extent[axis]) for axis in range(len(extent))]
    drawn = drawn.at[tuple(spot)].set(low)
    longest = extent.index(max(extent))
    spot[longest] = (spot[longest] + 1) % extent[longest]
    return drawn.at[tuple(spot)].set(top_value)


def steps_of(key, dims, pieces, smallest, largest):
    def one(dim, parts):
        draws = jax.random.uniform(jax.random.fold_in(jax.random.fold_in(key, 6), dim), (parts,), jnp.float32, smallest / len(pieces), largest / len(pieces))
        return jnp.repeat(jnp.exp(draws), dims[dim] // parts).reshape((-1,) + (1,) * (len(dims) - dim - 1))

    level = one(*pieces[0])
    for cut in pieces[1:]:
        level = level * one(*cut)
    return level


def setup_inputs(seed: int = 0) -> dict:
    keys = jax.random.split(jax.random.key(seed), 4)
    return {
        "ranks": jnp.clip(1.0 + 1.0 * jax.random.uniform(keys[0], (NZ, NY, NX), jnp.float32) ** steps_of(keys[0], (NZ, NY, NX), ((0, 32), (1, 8)), -0.2, 0.2), 1.0, 2.0),
        "seeds": jnp.clip(jnp.exp(math.log(1.0) - 1.3862944 * jax.random.uniform(keys[1], (3, NZ, NY, NX), jnp.float32) ** steps_of(keys[1], (3, NZ, NY, NX), ((1, 32), (2, 8)), -0.2, 0.2)), 0.25, 1.0),
        "flags": set_ends((jax.random.randint(keys[2], (NZ, NY, NX), 0, 8) < 1).astype(jnp.int32), jax.random.fold_in(keys[2], 1), 0, 1),
    }


def beside_all(ext, fill):
    wide = jnp.pad(ext, ((0, 0), (0, 0), (1, 1)), constant_values=fill)
    return [wide[1:-1, 1:-1, 2:], wide[1:-1, 1:-1, :-2], wide[1:-1, 2:, 1:-1],
            wide[1:-1, :-2, 1:-1], wide[2:, 1:-1, 1:-1], wide[:-2, 1:-1, 1:-1]]


def cycle(field, width, fill):
    return jnp.pad(field, ((width, width), (width, width), (0, 0)), constant_values=fill)


def bit_of(bits, number):
    return (bits // (2 ** number)) % 2


def select(packed_ext, bits):
    center = packed_ext[1:-1, 1:-1]
    values = beside_all(packed_ext, -3.0)
    nearest = jnp.full(center.shape, -3.0, center.dtype)
    for direction in range(6):
        linked = (bit_of(bits, direction) + bit_of(bits, direction + 6)) > 0
        nearest = jnp.maximum(nearest, jnp.where(linked, values[direction], -3.0))
    return ((center >= 0) & (center > nearest)).astype(jnp.int32)


def finer(coarse_ext, bits):
    values = beside_all(coarse_ext, 0)
    hit = jnp.zeros(bits.shape, jnp.int32)
    for direction in range(6):
        hit = hit + bit_of(bits, direction) * values[direction]
    return hit


def reference(ranks, seeds, flags):
    nz, ny, nx = ranks.shape
    zpos = jnp.arange(nz, dtype=jnp.int32)[:, None, None]
    ypos = jnp.arange(ny, dtype=jnp.int32)[None, :, None]
    xpos = jnp.arange(nx, dtype=jnp.int32)[None, None, :]
    zero = jnp.zeros((), jnp.float32)
    c0 = jnp.where(xpos < nx - 1, seeds[0], zero).astype(jnp.float32)
    c2 = jnp.where(ypos < ny - 1, seeds[1], zero).astype(jnp.float32)
    c4 = jnp.where(zpos < nz - 1, seeds[2], zero).astype(jnp.float32)
    c1 = jnp.pad(c0[:, :, :-1], ((0, 0), (0, 0), (1, 0)))
    c3 = jnp.pad(c2[:, :-1], ((0, 0), (1, 0), (0, 0)))
    c5 = jnp.pad(c4[:-1], ((1, 0), (0, 0), (0, 0)))
    couplings = [c0, c1, c2, c3, c4, c5]
    rowmax = c0
    for item in couplings[1:]:
        rowmax = jnp.maximum(rowmax, item)
    others = beside_all(cycle(rowmax, 1, 0.0), 0.0)
    bits = jnp.zeros(ranks.shape, jnp.int32)
    scale = jnp.ones(ranks.shape, jnp.float32)
    two = jnp.ones((), jnp.float32) * 2.0
    one = jnp.ones((), jnp.float32)
    for direction in range(6):
        cost = couplings[direction]
        depends = ((cost > 0) & (2.0 * cost >= rowmax)).astype(jnp.int32)
        feeds = ((cost > 0) & (2.0 * cost >= others[direction])).astype(jnp.int32)
        bits = bits + depends * (2 ** direction) + feeds * (2 ** (direction + 6))
        scale = scale * jnp.where(feeds == 1, two, one)
    measure = (ranks * scale).astype(jnp.float32)
    state = flags
    totals = []
    for step in range(ROUNDS):
        packed = jnp.where(state == 0, measure, jnp.where(state == 2, -2.0, -1.0)).astype(jnp.float32)
        coarse = select(cycle(packed, 1, 0.0), bits)
        hit = finer(cycle(coarse, 1, 0), bits)
        state = jnp.where(coarse == 1, 2, jnp.where((state == 0) & (hit > 0), 1, state)).astype(jnp.int32)
        totals.append(jnp.sum((state == 0).astype(jnp.int32)))
    return state, jnp.stack(totals).astype(jnp.int32)
```

```python
import functools

import jax
import jax.numpy as jnp
from jax import lax
from jax.experimental import pallas as pl
from jax.experimental.pallas import tpu as pltpu
from jax.sharding import PartitionSpec as P

ROUNDS = 3
MESH = pl.DeviceIdType.MESH
UP_UP, UP_DOWN, DOWN_UP, DOWN_DOWN = (1, 1), (1, -1), (-1, 1), (-1, -1)
DIAGONALS = (UP_UP, UP_DOWN, DOWN_UP, DOWN_DOWN)
DIRECTIONS = ((1, 0), (-1, 0), (0, 1), (0, -1)) + DIAGONALS
NONE = -3.0
LINK_Y, DEP_Y = 1 << 12, 1 << 13


def kernel(
    nz, ny,
    ranks_hbm, seeds_hbm, flags_hbm,
    state_ref, totals_ref,
    ranks, seeds, flags,
    bits, partial, rowmax, below, edge_y_out, edge_y_in, edge_d_out, edge_d_in,
    packed, near, near_halo, newc, row_out, row_in, diag_out, diag_in,
    column, whole,
    load_sem, edge_send, edge_recv, round_send, round_recv, col_send, col_recv, all_send, all_recv,
):
    gz, gy = lax.axis_index("gz"), lax.axis_index("gy")
    depth, rows, width = ranks.shape
    top, end = depth - 1, rows - 1

    loads = [
        pltpu.make_async_copy(seeds_hbm, seeds, load_sem.at[0]),
        pltpu.make_async_copy(ranks_hbm, ranks, load_sem.at[1]),
        pltpu.make_async_copy(flags_hbm, flags, load_sem.at[2]),
    ]
    for load in loads:
        load.start()

    def exists(dz, dy):
        here = None
        for at, step, count in ((gz, dz, nz), (gy, dy, ny)):
            if step:
                inside = at < count - 1 if step > 0 else at > 0
                here = inside if here is None else here & inside
        return here

    there = {d: exists(*d) for d in DIRECTIONS}
    target = {d: (gz + d[0], gy + d[1]) for d in DIRECTIONS}

    barrier = pltpu.get_barrier_semaphore()
    for d in DIAGONALS:
        @pl.when(there[d])
        def _(d=d):
            pl.semaphore_signal(barrier, inc=1, device_id=target[d], device_id_type=MESH)

    @pl.loop(1, nz)
    def _(k):
        pl.semaphore_signal(barrier, inc=1, device_id=(lax.rem(gz + k, nz), gy), device_id_type=MESH)

    @pl.loop(1, ny)
    def _(k):
        pl.semaphore_signal(barrier, inc=1, device_id=(gz, lax.rem(gy + k, ny)), device_id_type=MESH)

    def one(flag):
        return jnp.where(flag, 1, 0).astype(jnp.int32)

    sides_z = one(there[(1, 0)]) + one(there[(-1, 0)])
    sides_y = one(there[(0, 1)]) + one(there[(0, -1)])

    def fill(direction, *refs_values):
        @pl.when(jnp.logical_not(there[direction]))
        def _():
            for ref, value in refs_values:
                ref[...] = jnp.full(ref.shape, value, ref.dtype)

    fill((-1, 0), (below, 0.0), (partial.at[0], 0.0), *[(packed.at[r, 0], NONE) for r in range(ROUNDS)],
         *[(near_halo.at[r, 0], NONE) for r in range(ROUNDS)])
    fill((1, 0), (partial.at[depth + 1], 0.0), *[(packed.at[r, depth + 1], NONE) for r in range(ROUNDS)],
         *[(near_halo.at[r, 1], NONE) for r in range(ROUNDS)])
    fill((0, -1), (edge_y_in.at[0:2], 0.0), *[(row_in.at[r, 0], NONE) for r in range(ROUNDS)])
    fill((0, 1), (edge_y_in.at[2:3], 0.0), *[(row_in.at[r, 1], NONE) for r in range(ROUNDS)])
    fill(DOWN_DOWN, (edge_d_in.at[0:2], 0.0))
    fill(DOWN_UP, (edge_d_in.at[2:3], 0.0))
    fill(UP_DOWN, (edge_d_in.at[3:4], 0.0))
    for i, d in enumerate(DIAGONALS):
        fill((-d[0], -d[1]), *[(diag_in.at[r, i], NONE) for r in range(ROUNDS)])

    pl.semaphore_wait(barrier, nz - 1 + ny - 1 + sides_z * sides_y)

    started = []

    def remote(direction, source, target_ref, send, recv):
        copy = pltpu.make_async_remote_copy(
            src_ref=source, dst_ref=target_ref, send_sem=send, recv_sem=recv,
            device_id=target[direction], device_id_type=MESH,
        )

        @pl.when(there[direction])
        def _():
            copy.start()

        started.append((direction, copy))
        return direction, copy

    def arrived(pair):
        (dz, dy), copy = pair

        @pl.when(there[(-dz, -dy)])
        def _():
            copy.wait_recv()

    xpos = lax.broadcasted_iota(jnp.int32, (rows, width), 1)
    ypos = lax.broadcasted_iota(jnp.int32, (rows, width), 0)
    first, last = ypos == 0, ypos == end

    def over(row, where, plane):
        return jnp.where(where, jnp.broadcast_to(row, plane.shape), plane)

    def east(plane):
        return pltpu.roll(plane, width - 1, 1)

    def west(plane):
        return pltpu.roll(plane, 1, 1)

    def north(plane):
        return pltpu.roll(plane, rows - 1, 0)

    def south(plane):
        return pltpu.roll(plane, 1, 0)

    zero = jnp.zeros((rows, width), jnp.float32)

    loads[0].wait()

    def in_plane(z):
        c0 = jnp.where(xpos < width - 1, seeds[0, z], 0.0)
        c2 = jnp.where(last & (gy == ny - 1), 0.0, seeds[1, z])
        c4 = seeds[2, z]
        c4 = jnp.where((gz == nz - 1) & (z == top), zero, c4)
        return c0, c2, c4

    def part(z):
        c0, c2, c4 = in_plane(z)
        m = jnp.maximum(jnp.maximum(c0, west(c0)), jnp.maximum(c2, c4))
        m = jnp.maximum(m, jnp.where(first, 0.0, south(c2)))
        if not isinstance(z, int) or z > 0:
            m = jnp.maximum(m, seeds[2, z - 1])
        partial[z + 1] = m
        edge_y_out[0, z] = seeds[1, z, end:rows, :]
        edge_y_out[1, z] = m[end:rows]
        edge_y_out[2, z] = m[0:1]

    edges = [remote((1, 0), seeds.at[2, top], below, edge_send.at[0], edge_recv.at[0])]
    part(top)
    edges.append(remote((1, 0), partial.at[depth], partial.at[0], edge_send.at[1], edge_recv.at[1]))
    part(0)
    edges.append(remote((-1, 0), partial.at[1], partial.at[depth + 1], edge_send.at[2], edge_recv.at[2]))
    edge_d_out[0] = seeds[1, top, end:rows, :]
    edge_d_out[1] = seeds[2, top, end:rows, :]
    edge_d_out[2] = seeds[2, top, 0:1, :]
    edge_d_out[3] = seeds[1, 0, end:rows, :]
    for z in range(1, top):
        part(z)
    edges.append(remote((0, 1), edge_y_out.at[0:2], edge_y_in.at[0:2], edge_send.at[3], edge_recv.at[3]))
    edges.append(remote((0, -1), edge_y_out.at[2:3], edge_y_in.at[2:3], edge_send.at[4], edge_recv.at[4]))
    edges.append(remote(UP_UP, edge_d_out.at[0:2], edge_d_in.at[0:2], edge_send.at[5], edge_recv.at[5]))
    edges.append(remote(UP_DOWN, edge_d_out.at[2:3], edge_d_in.at[2:3], edge_send.at[6], edge_recv.at[6]))
    edges.append(remote(DOWN_UP, edge_d_out.at[3:4], edge_d_in.at[3:4], edge_send.at[7], edge_recv.at[7]))

    loads[1].wait()
    loads[2].wait()
    for pair in edges:
        arrived(pair)

    for z in range(depth):
        m = jnp.maximum(partial[z + 1], jnp.where(first, jnp.broadcast_to(edge_y_in[0, z], zero.shape), 0.0))
        if z == 0:
            m = jnp.maximum(m, below[...])
        rowmax[z + 1] = m
    m = partial[0]
    rowmax[0] = jnp.maximum(m, jnp.where(first, jnp.broadcast_to(edge_d_in[0], zero.shape), 0.0))
    m = jnp.maximum(partial[depth + 1], in_plane(top)[2])
    rowmax[depth + 1] = jnp.maximum(m, jnp.where(first, jnp.broadcast_to(edge_d_in[3], zero.shape), 0.0))

    def strengths(z):
        c0, c2, c4 = in_plane(z)
        c1 = west(c0)
        c3 = over(edge_y_in[0, z], first, south(c2))
        c5 = below[...] if z == 0 else seeds[2, z - 1]
        mine = rowmax[z + 1]
        low = edge_y_in[1, z]
        high = jnp.maximum(edge_y_in[2, z], c2[end:rows])
        if z == 0:
            low = jnp.maximum(low, edge_d_in[1])
            high = jnp.maximum(high, edge_d_in[2])
        others = [
            east(mine), west(mine), over(high, last, north(mine)), over(low, first, south(mine)),
            rowmax[z + 2], rowmax[z],
        ]
        word = jnp.zeros((rows, width), jnp.int32)
        measure = ranks[z]
        outer_link = outer_dep = None
        for d, (cost, other) in enumerate(zip((c0, c1, c2, c3, c4, c5), others)):
            twice = 2.0 * cost
            depends = (cost > 0) & (twice >= mine)
            feeds = (cost > 0) & (twice >= other)
            measure = jnp.where(feeds, 2.0 * measure, measure)
            link = depends | feeds
            if d in (2, 3):
                border = last if d == 2 else first
                outer = jnp.where(link & border, LINK_Y, 0) + jnp.where(depends & border, DEP_Y, 0)
                word = word + outer
                link = link & jnp.logical_not(border)
                depends = depends & jnp.logical_not(border)
            word = word + jnp.where(link, 1 << d, 0) + jnp.where(depends, 1 << (d + 6), 0)
        bits[z] = word
        flag = flags[z]
        packed[0, z + 1] = jnp.where(flag == 0, measure, jnp.where(flag == 2, -2.0, -1.0))

    def linked(word, mask, value):
        return jnp.where((word & mask) != 0, value, NONE)

    def near_inside(r, z):
        word, here = bits[z], packed[r, z + 1]
        m = jnp.maximum(linked(word, 1, east(here)), linked(word, 2, west(here)))
        m = jnp.maximum(m, linked(word, 4, north(here)))
        m = jnp.maximum(m, linked(word, 8, south(here)))
        if z < top:
            m = jnp.maximum(m, linked(word, 16, packed[r, z + 2]))
        if z > 0:
            m = jnp.maximum(m, linked(word, 32, packed[r, z]))
        near[r, z] = m
        for arr, plane in ((0, here), (1, m)):
            row_out[r, 0, arr, z] = plane[end:rows]
            row_out[r, 1, arr, z] = plane[0:1]

    def corner(r, i, d):
        z, row, z_mask = (top if d[0] > 0 else 0), (end if d[1] > 0 else 0), (16 if d[0] > 0 else 32)
        word, value = bits[z, row : row + 1, :], packed[r, z + 1, row : row + 1, :]
        diag_out[r, i, 0] = linked(word, LINK_Y, value)
        diag_out[r, i, 1] = linked(word, z_mask, value)

    def exchange(r):
        send, recv = round_send.at[r], round_recv.at[r]
        near_inside(r, top)
        near_inside(r, 0)
        copies = [
            remote((1, 0), packed.at[r, depth], packed.at[r, 0], send.at[0], recv.at[0]),
            remote((1, 0), near.at[r, top], near_halo.at[r, 0], send.at[1], recv.at[1]),
            remote((-1, 0), packed.at[r, 1], packed.at[r, depth + 1], send.at[2], recv.at[2]),
            remote((-1, 0), near.at[r, 0], near_halo.at[r, 1], send.at[3], recv.at[3]),
        ]
        for i, d in enumerate(DIAGONALS):
            corner(r, i, d)
            copies.append(remote(d, diag_out.at[r, i], diag_in.at[r, i], send.at[6 + i], recv.at[6 + i]))
        for z in range(1, top):
            near_inside(r, z)
        copies.append(remote((0, 1), row_out.at[r, 0], row_in.at[r, 0], send.at[4], recv.at[4]))
        copies.append(remote((0, -1), row_out.at[r, 1], row_in.at[r, 1], send.at[5], recv.at[5]))
        for pair in copies:
            arrived(pair)

    def yes(mask):
        return jnp.where(mask, -1, 0).astype(jnp.int32)

    def halo_rows(r, arr, z):
        low = jnp.broadcast_to(row_in[r, 0, arr, z], (rows, width))
        return over(row_in[r, 1, arr, z], last, low)

    def finish_near(r, z):
        word, here = bits[z], packed[r, z + 1]
        m = jnp.maximum(near[r, z], linked(word, LINK_Y, halo_rows(r, 0, z)))
        if z == top:
            m = jnp.maximum(m, linked(word, 16, packed[r, z + 2]))
        if z == 0:
            m = jnp.maximum(m, linked(word, 32, packed[r, z]))
        newc[z + 1] = yes((here >= 0) & (here > m))

    def outside_z(r, low):
        z, at, mask = (0, 0, 32) if low else (top, depth + 1, 16)
        there_packed, mine = packed[r, at], packed[r, z + 1]
        limit = jnp.maximum(near_halo[r, 0 if low else 1], linked(bits[z], mask, mine))
        i, j = (0, 1) if low else (2, 3)
        limit = jnp.where(first, jnp.maximum(limit, jnp.broadcast_to(diag_in[r, i, 0], limit.shape)), limit)
        limit = jnp.where(last, jnp.maximum(limit, jnp.broadcast_to(diag_in[r, j, 0], limit.shape)), limit)
        newc[at] = yes((there_packed >= 0) & (there_packed > limit))

    def update(r, z, count):
        word, here, chosen = bits[z], packed[r, z + 1], newc[z + 1]
        outer, limit = halo_rows(r, 0, z), halo_rows(r, 1, z)
        limit = jnp.maximum(limit, linked(word, LINK_Y, here))
        if z in (0, top):
            i, j = (0, 1) if z == 0 else (2, 3)
            corner_value = over(diag_in[r, j, 1], last, jnp.broadcast_to(diag_in[r, i, 1], (rows, width)))
            limit = jnp.maximum(limit, corner_value)
        hit = word & DEP_Y & yes((outer >= 0) & (outer > limit))
        for d, value in enumerate((east(chosen), west(chosen), north(chosen), south(chosen), newc[z + 2], newc[z])):
            hit = hit | (word & (1 << (d + 6)) & value)
        after = jnp.where(chosen != 0, -2.0, jnp.where((here >= 0) & (hit != 0), -1.0, here))
        if r + 1 < ROUNDS:
            packed[r + 1, z + 1] = after
        else:
            state_ref[z] = jnp.where(after >= 0, 0, jnp.where(after == -2.0, 2, 1)).astype(jnp.int32)
        return count + jnp.where(after >= 0, 1.0, 0.0)

    for z in range(depth):
        strengths(z)

    lane = lax.broadcasted_iota(jnp.int32, (1, 128), 1)
    counted = jnp.zeros((1, 128), jnp.float32)
    for r in range(ROUNDS):
        exchange(r)
        outside_z(r, True)
        outside_z(r, False)
        for z in range(depth):
            finish_near(r, z)
        count = zero
        for z in range(depth):
            count = update(r, z, count)
        counted = jnp.where(lane == r, jnp.sum(count), counted)

    column[gy] = counted

    def col_copy(k):
        return pltpu.make_async_remote_copy(
            src_ref=column.at[gy], dst_ref=column.at[gy], send_sem=col_send.at[k], recv_sem=col_recv.at[gy],
            device_id=(gz, lax.rem(gy + k, ny)), device_id_type=MESH)

    def all_copy(k):
        return pltpu.make_async_remote_copy(
            src_ref=whole.at[gz], dst_ref=whole.at[gz], send_sem=all_send.at[k], recv_sem=all_recv.at[gz],
            device_id=(lax.rem(gz + k, nz), gy), device_id_type=MESH)

    def landed(buffer, sem, me, count):
        @pl.loop(1, count)
        def _(k):
            who = lax.rem(me + k, count)
            pltpu.make_async_copy(buffer.at[who], buffer.at[who], sem.at[who]).wait()

    @pl.loop(1, ny)
    def _(k):
        col_copy(k).start()

    landed(column, col_recv, gy, ny)
    whole[gz] = jnp.sum(column[...], axis=0)

    @pl.loop(1, nz)
    def _(k):
        all_copy(k).start()

    landed(whole, all_recv, gz, nz)
    totals_ref[...] = jnp.sum(whole[...], axis=0).astype(jnp.int32)

    for (dz, dy), copy in started:
        @pl.when(there[(dz, dy)])
        def _(copy=copy):
            copy.wait_send()

    @pl.loop(1, ny)
    def _(k):
        col_copy(k).wait_send()

    @pl.loop(1, nz)
    def _(k):
        all_copy(k).wait_send()


def per_device(nz, ny, ranks, seeds, flags):
    depth, rows, width = ranks.shape
    f32, i32, vmem, dma = jnp.float32, jnp.int32, pltpu.VMEM, pltpu.SemaphoreType.DMA
    plane = (rows, width)
    scratch = [
        vmem(ranks.shape, f32), vmem(seeds.shape, f32), vmem(flags.shape, i32),
        vmem(ranks.shape, i32), vmem((depth + 2, *plane), f32), vmem((depth + 2, *plane), f32), vmem(plane, f32),
        vmem((3, depth, 1, width), f32), vmem((3, depth, 1, width), f32),
        vmem((4, 1, width), f32), vmem((4, 1, width), f32),
        vmem((ROUNDS, depth + 2, *plane), f32), vmem((ROUNDS, depth, *plane), f32), vmem((ROUNDS, 2, *plane), f32),
        vmem((depth + 2, *plane), i32),
        vmem((ROUNDS, 2, 2, depth, 1, width), f32), vmem((ROUNDS, 2, 2, depth, 1, width), f32),
        vmem((ROUNDS, 4, 2, 1, width), f32), vmem((ROUNDS, 4, 2, 1, width), f32),
        vmem((ny, 1, 128), f32), vmem((nz, 1, 128), f32),
        dma((3,)), dma((8,)), dma((8,)), dma((ROUNDS, 10)), dma((ROUNDS, 10)),
        dma((ny,)), dma((ny,)), dma((nz,)), dma((nz,)),
    ]
    state, totals = pl.pallas_call(
        functools.partial(kernel, nz, ny),
        out_shape=(jax.ShapeDtypeStruct(ranks.shape, i32), jax.ShapeDtypeStruct((1, 128), i32)),
        in_specs=[pl.BlockSpec(memory_space=pl.ANY)] * 3,
        out_specs=(pl.BlockSpec(memory_space=pltpu.VMEM), pl.BlockSpec(memory_space=pltpu.VMEM)),
        scratch_shapes=scratch,
        compiler_params=pltpu.CompilerParams(collective_id=0, has_side_effects=True),
    )(ranks, seeds, flags)
    return state, totals[0, :ROUNDS]


def solution(mesh):
    nz, ny = mesh.shape["gz"], mesh.shape["gy"]
    return jax.shard_map(
        functools.partial(per_device, nz, ny), mesh=mesh,
        in_specs=(P("gz", "gy", None), P(None, "gz", "gy", None), P("gz", "gy", None)),
        out_specs=(P("gz", "gy", None), P()), check_vma=False,
    )
```

```python
import functools

import jax
import jax.numpy as jnp
from jax import lax
from jax.experimental import pallas as pl
from jax.experimental.pallas import tpu as pltpu
from jax.sharding import PartitionSpec as P

ROUNDS = 3
MESH = pl.DeviceIdType.MESH
UP_UP, UP_DOWN, DOWN_UP, DOWN_DOWN = (1, 1), (1, -1), (-1, 1), (-1, -1)
DIAGONALS = (UP_UP, UP_DOWN, DOWN_UP, DOWN_DOWN)
DIRECTIONS = ((1, 0), (-1, 0), (0, 1), (0, -1)) + DIAGONALS
NONE = -3.0
LINK_Y, DEP_Y = 1 << 12, 1 << 13


def kernel(
    nz, ny,
    ranks_hbm, seeds_hbm, flags_hbm,
    state_ref, totals_ref,
    ranks, seeds, flags,
    bits, partial, rowmax, below, edge_y_out, edge_y_in, edge_d_out, edge_d_in,
    packed, near, near_halo, newc, row_out, row_in, diag_out, diag_in,
    column, whole,
    known, load_sem, edge_send, edge_recv, round_send, round_recv, col_send, col_recv, all_send, all_recv,
):
    gz, gy = lax.axis_index("gz"), lax.axis_index("gy")
    depth, rows, width = ranks.shape
    top, end = depth - 1, rows - 1

    loads = [
        pltpu.make_async_copy(seeds_hbm, seeds, load_sem.at[0]),
        pltpu.make_async_copy(ranks_hbm, ranks, load_sem.at[1]),
        pltpu.make_async_copy(flags_hbm, flags, load_sem.at[2]),
    ]
    for load in loads:
        load.start()

    def exists(dz, dy):
        here = None
        for at, step, count in ((gz, dz, nz), (gy, dy, ny)):
            if step:
                inside = at < count - 1 if step > 0 else at > 0
                here = inside if here is None else here & inside
        return here

    there = {d: exists(*d) for d in DIRECTIONS}
    target = {d: (gz + d[0], gy + d[1]) for d in DIRECTIONS}

    barrier = pltpu.get_barrier_semaphore()
    for d in DIAGONALS:
        @pl.when(there[d])
        def _(d=d):
            pl.semaphore_signal(barrier, inc=1, device_id=target[d], device_id_type=MESH)

    for step in (1, nz - 1):
        pl.semaphore_signal(barrier, inc=1, device_id=(lax.rem(gz + step, nz), gy), device_id_type=MESH)

    @pl.loop(1, ny)
    def _(k):
        pl.semaphore_signal(barrier, inc=1, device_id=(gz, lax.rem(gy + k, ny)), device_id_type=MESH)

    strides, reach = [], 1
    while 2 * reach + 1 < nz:
        strides.append(reach)
        reach *= 2

    def tell(i):
        if i < len(strides):
            for step in (strides[i], nz - strides[i]):
                pl.semaphore_signal(known.at[i], inc=1, device_id=(lax.rem(gz + step, nz), gy), device_id_type=MESH)

    def told(i):
        if i < len(strides):
            pl.semaphore_wait(known.at[i], 2)

    def one(flag):
        return jnp.where(flag, 1, 0).astype(jnp.int32)

    sides_z = one(there[(1, 0)]) + one(there[(-1, 0)])
    sides_y = one(there[(0, 1)]) + one(there[(0, -1)])

    started = []

    def remote(direction, source, target_ref, send, recv):
        copy = pltpu.make_async_remote_copy(
            src_ref=source, dst_ref=target_ref, send_sem=send, recv_sem=recv,
            device_id=target[direction], device_id_type=MESH,
        )

        @pl.when(there[direction])
        def _():
            copy.start()

        started.append((direction, copy))
        return direction, copy

    def arrived(pair):
        (dz, dy), copy = pair

        @pl.when(there[(-dz, -dy)])
        def _():
            copy.wait_recv()

    xpos = lax.broadcasted_iota(jnp.int32, (rows, width), 1)
    ypos = lax.broadcasted_iota(jnp.int32, (rows, width), 0)
    first, last = ypos == 0, ypos == end

    def over(row, where, plane):
        return jnp.where(where, jnp.broadcast_to(row, plane.shape), plane)

    def east(plane):
        return pltpu.roll(plane, width - 1, 1)

    def west(plane):
        return pltpu.roll(plane, 1, 1)

    def north(plane):
        return pltpu.roll(plane, rows - 1, 0)

    def south(plane):
        return pltpu.roll(plane, 1, 0)

    zero = jnp.zeros((rows, width), jnp.float32)

    loads[0].wait()

    def in_plane(z):
        c0 = jnp.where(xpos < width - 1, seeds[0, z], 0.0)
        c2 = jnp.where(last & (gy == ny - 1), 0.0, seeds[1, z])
        c4 = seeds[2, z]
        c4 = jnp.where((gz == nz - 1) & (z == top), zero, c4)
        return c0, c2, c4

    def part(z):
        c0, c2, c4 = in_plane(z)
        m = jnp.maximum(jnp.maximum(c0, west(c0)), jnp.maximum(c2, c4))
        m = jnp.maximum(m, jnp.where(first, 0.0, south(c2)))
        if not isinstance(z, int) or z > 0:
            m = jnp.maximum(m, seeds[2, z - 1])
        partial[z + 1] = m
        edge_y_out[0, z] = seeds[1, z, end:rows, :]
        edge_y_out[1, z] = m[end:rows]
        edge_y_out[2, z] = m[0:1]

    part(top)
    part(0)
    edge_d_out[0] = seeds[1, top, end:rows, :]
    edge_d_out[1] = seeds[2, top, end:rows, :]
    edge_d_out[2] = seeds[2, top, 0:1, :]
    edge_d_out[3] = seeds[1, 0, end:rows, :]

    pl.semaphore_wait(barrier, 2 + ny - 1 + sides_z * sides_y)

    def edge(direction, source, target_ref, i):
        return remote(direction, source, target_ref, edge_send.at[i], edge_recv.at[i])

    edge_d = [
        edge(UP_UP, edge_d_out.at[0:2], edge_d_in.at[0:2], 0),
        edge(UP_DOWN, edge_d_out.at[2:3], edge_d_in.at[2:3], 1),
        edge(DOWN_UP, edge_d_out.at[3:4], edge_d_in.at[3:4], 2),
    ]
    edge_z = [
        edge((1, 0), seeds.at[2, top], below, 3),
        edge((1, 0), partial.at[depth], partial.at[0], 4),
        edge((-1, 0), partial.at[1], partial.at[depth + 1], 5),
    ]
    tell(0)
    for z in range(1, top):
        part(z)
    edge_y = [
        edge((0, 1), edge_y_out.at[0:2], edge_y_in.at[0:2], 6),
        edge((0, -1), edge_y_out.at[2:3], edge_y_in.at[2:3], 7),
    ]

    def fill(direction, *refs_values):
        @pl.when(jnp.logical_not(there[direction]))
        def _():
            for ref, value in refs_values:
                ref[...] = jnp.full(ref.shape, value, ref.dtype)

    fill((-1, 0), (below, 0.0), (partial.at[0], 0.0), *[(packed.at[r, 0], NONE) for r in range(ROUNDS)],
         *[(near_halo.at[r, 0], NONE) for r in range(ROUNDS)])
    fill((1, 0), (partial.at[depth + 1], 0.0), *[(packed.at[r, depth + 1], NONE) for r in range(ROUNDS)],
         *[(near_halo.at[r, 1], NONE) for r in range(ROUNDS)])
    fill((0, -1), (edge_y_in.at[0:2], 0.0), *[(row_in.at[r, 0], NONE) for r in range(ROUNDS)])
    fill((0, 1), (edge_y_in.at[2:3], 0.0), *[(row_in.at[r, 1], NONE) for r in range(ROUNDS)])
    fill(DOWN_DOWN, (edge_d_in.at[0:2], 0.0))
    fill(DOWN_UP, (edge_d_in.at[2:3], 0.0))
    fill(UP_DOWN, (edge_d_in.at[3:4], 0.0))
    for i, d in enumerate(DIAGONALS):
        fill((-d[0], -d[1]), *[(diag_in.at[r, i], NONE) for r in range(ROUNDS)])

    def whole_rowmax(z):
        m = jnp.maximum(partial[z + 1], jnp.where(first, jnp.broadcast_to(edge_y_in[0, z], zero.shape), 0.0))
        if z == 0:
            m = jnp.maximum(m, below[...])
        rowmax[z + 1] = m

    def outside_rowmax():
        m = partial[0]
        rowmax[0] = jnp.maximum(m, jnp.where(first, jnp.broadcast_to(edge_d_in[0], zero.shape), 0.0))
        m = jnp.maximum(partial[depth + 1], in_plane(top)[2])
        rowmax[depth + 1] = jnp.maximum(m, jnp.where(first, jnp.broadcast_to(edge_d_in[3], zero.shape), 0.0))

    def strengths(z):
        c0, c2, c4 = in_plane(z)
        c1 = west(c0)
        c3 = over(edge_y_in[0, z], first, south(c2))
        c5 = below[...] if z == 0 else seeds[2, z - 1]
        mine = rowmax[z + 1]
        low = edge_y_in[1, z]
        high = jnp.maximum(edge_y_in[2, z], c2[end:rows])
        if z == 0:
            low = jnp.maximum(low, edge_d_in[1])
            high = jnp.maximum(high, edge_d_in[2])
        others = [
            east(mine), west(mine), over(high, last, north(mine)), over(low, first, south(mine)),
            rowmax[z + 2], rowmax[z],
        ]
        word = jnp.zeros((rows, width), jnp.int32)
        measure = ranks[z]
        outer_link = outer_dep = None
        for d, (cost, other) in enumerate(zip((c0, c1, c2, c3, c4, c5), others)):
            twice = 2.0 * cost
            depends = (cost > 0) & (twice >= mine)
            feeds = (cost > 0) & (twice >= other)
            measure = jnp.where(feeds, 2.0 * measure, measure)
            link = depends | feeds
            if d in (2, 3):
                border = last if d == 2 else first
                outer = jnp.where(link & border, LINK_Y, 0) + jnp.where(depends & border, DEP_Y, 0)
                word = word + outer
                link = link & jnp.logical_not(border)
                depends = depends & jnp.logical_not(border)
            word = word + jnp.where(link, 1 << d, 0) + jnp.where(depends, 1 << (d + 6), 0)
        bits[z] = word
        flag = flags[z]
        packed[0, z + 1] = jnp.where(flag == 0, measure, jnp.where(flag == 2, -2.0, -1.0))

    def linked(word, mask, value):
        return jnp.where((word & mask) != 0, value, NONE)

    def near_inside(r, z):
        word, here = bits[z], packed[r, z + 1]
        m = jnp.maximum(linked(word, 1, east(here)), linked(word, 2, west(here)))
        m = jnp.maximum(m, linked(word, 4, north(here)))
        m = jnp.maximum(m, linked(word, 8, south(here)))
        if z < top:
            m = jnp.maximum(m, linked(word, 16, packed[r, z + 2]))
        if z > 0:
            m = jnp.maximum(m, linked(word, 32, packed[r, z]))
        near[r, z] = m
        for arr, plane in ((0, here), (1, m)):
            row_out[r, 0, arr, z] = plane[end:rows]
            row_out[r, 1, arr, z] = plane[0:1]

    def corner(r, i, d):
        z, row, z_mask = (top if d[0] > 0 else 0), (end if d[1] > 0 else 0), (16 if d[0] > 0 else 32)
        word, value = bits[z, row : row + 1, :], packed[r, z + 1, row : row + 1, :]
        diag_out[r, i, 0] = linked(word, LINK_Y, value)
        diag_out[r, i, 1] = linked(word, z_mask, value)

    def send_packed(r):
        send, recv = round_send.at[r], round_recv.at[r]
        for i, d in enumerate(DIAGONALS):
            corner(r, i, d)
        return [
            *[remote(d, diag_out.at[r, i], diag_in.at[r, i], send.at[6 + i], recv.at[6 + i]) for i, d in enumerate(DIAGONALS)],
            remote((1, 0), packed.at[r, depth], packed.at[r, 0], send.at[0], recv.at[0]),
            remote((-1, 0), packed.at[r, 1], packed.at[r, depth + 1], send.at[2], recv.at[2]),
        ]

    def send_near(r):
        send, recv = round_send.at[r], round_recv.at[r]
        return [
            remote((1, 0), near.at[r, top], near_halo.at[r, 0], send.at[1], recv.at[1]),
            remote((-1, 0), near.at[r, 0], near_halo.at[r, 1], send.at[3], recv.at[3]),
        ]

    def send_rows(r):
        send, recv = round_send.at[r], round_recv.at[r]
        return [
            remote((0, 1), row_out.at[r, 0], row_in.at[r, 0], send.at[4], recv.at[4]),
            remote((0, -1), row_out.at[r, 1], row_in.at[r, 1], send.at[5], recv.at[5]),
        ]

    def yes(mask):
        return jnp.where(mask, -1, 0).astype(jnp.int32)

    def halo_rows(r, arr, z):
        low = jnp.broadcast_to(row_in[r, 0, arr, z], (rows, width))
        return over(row_in[r, 1, arr, z], last, low)

    def finish_near(r, z):
        word, here = bits[z], packed[r, z + 1]
        m = jnp.maximum(near[r, z], linked(word, LINK_Y, halo_rows(r, 0, z)))
        if z == top:
            m = jnp.maximum(m, linked(word, 16, packed[r, z + 2]))
        if z == 0:
            m = jnp.maximum(m, linked(word, 32, packed[r, z]))
        newc[z + 1] = yes((here >= 0) & (here > m))

    def outside_z(r, low):
        z, at, mask = (0, 0, 32) if low else (top, depth + 1, 16)
        there_packed, mine = packed[r, at], packed[r, z + 1]
        limit = jnp.maximum(near_halo[r, 0 if low else 1], linked(bits[z], mask, mine))
        i, j = (0, 1) if low else (2, 3)
        limit = jnp.where(first, jnp.maximum(limit, jnp.broadcast_to(diag_in[r, i, 0], limit.shape)), limit)
        limit = jnp.where(last, jnp.maximum(limit, jnp.broadcast_to(diag_in[r, j, 0], limit.shape)), limit)
        newc[at] = yes((there_packed >= 0) & (there_packed > limit))

    def update(r, z, count):
        word, here, chosen = bits[z], packed[r, z + 1], newc[z + 1]
        outer, limit = halo_rows(r, 0, z), halo_rows(r, 1, z)
        limit = jnp.maximum(limit, linked(word, LINK_Y, here))
        if z in (0, top):
            i, j = (0, 1) if z == 0 else (2, 3)
            corner_value = over(diag_in[r, j, 1], last, jnp.broadcast_to(diag_in[r, i, 1], (rows, width)))
            limit = jnp.maximum(limit, corner_value)
        hit = word & DEP_Y & yes((outer >= 0) & (outer > limit))
        for d, value in enumerate((east(chosen), west(chosen), north(chosen), south(chosen), newc[z + 2], newc[z])):
            hit = hit | (word & (1 << (d + 6)) & value)
        after = jnp.where(chosen != 0, -2.0, jnp.where((here >= 0) & (hit != 0), -1.0, here))
        if r + 1 < ROUNDS:
            packed[r + 1, z + 1] = after
        else:
            state_ref[z] = jnp.where(after >= 0, 0, jnp.where(after == -2.0, 2, 1)).astype(jnp.int32)
        return count + jnp.where(after >= 0, 1.0, 0.0)

    def wait_all(pairs):
        for pair in pairs:
            arrived(pair)

    inner, middle = range(1, top), range(2, top - 1)
    loads[1].wait()
    loads[2].wait()
    wait_all(edge_y)
    for z in inner:
        whole_rowmax(z)
    for z in middle:
        strengths(z)
    wait_all(edge_z)
    wait_all(edge_d)
    whole_rowmax(0)
    whole_rowmax(top)
    outside_rowmax()
    strengths(0)
    strengths(top)
    told(0)
    tell(1)

    lane = lax.broadcasted_iota(jnp.int32, (1, 128), 1)
    counted = jnp.zeros((1, 128), jnp.float32)
    for r in range(ROUNDS):
        sent_packed = send_packed(r)
        if r == 0:
            strengths(1)
            strengths(top - 1)
        near_inside(r, 0)
        near_inside(r, top)
        sent_near = send_near(r)
        for z in inner:
            near_inside(r, z)
        sent_rows = send_rows(r)

        wait_all(sent_rows)
        for z in inner:
            finish_near(r, z)
        count = zero
        for z in middle:
            count = update(r, z, count)
        wait_all(sent_packed)
        finish_near(r, 0)
        finish_near(r, top)
        count = update(r, 1, count)
        count = update(r, top - 1, count)
        wait_all(sent_near)
        outside_z(r, True)
        outside_z(r, False)
        count = update(r, 0, count)
        count = update(r, top, count)
        told(r + 1)
        tell(r + 2)
        counted = jnp.where(lane == r, jnp.sum(count), counted)

    column[gy] = counted

    def col_copy(k):
        return pltpu.make_async_remote_copy(
            src_ref=column.at[gy], dst_ref=column.at[gy], send_sem=col_send.at[k], recv_sem=col_recv.at[gy],
            device_id=(gz, lax.rem(gy + k, ny)), device_id_type=MESH)

    def all_copy(k):
        return pltpu.make_async_remote_copy(
            src_ref=whole.at[gz], dst_ref=whole.at[gz], send_sem=all_send.at[k], recv_sem=all_recv.at[gz],
            device_id=(lax.rem(gz + k, nz), gy), device_id_type=MESH)

    def landed(buffer, sem, me, count):
        @pl.loop(1, count)
        def _(k):
            who = lax.rem(me + k, count)
            pltpu.make_async_copy(buffer.at[who], buffer.at[who], sem.at[who]).wait()

    @pl.loop(1, ny)
    def _(k):
        col_copy(k).start()

    landed(column, col_recv, gy, ny)
    whole[gz] = jnp.sum(column[...], axis=0)

    @pl.loop(1, nz)
    def _(k):
        all_copy(k).start()

    landed(whole, all_recv, gz, nz)
    totals_ref[...] = jnp.sum(whole[...], axis=0)

    for (dz, dy), copy in started:
        @pl.when(there[(dz, dy)])
        def _(copy=copy):
            copy.wait_send()

    @pl.loop(1, ny)
    def _(k):
        col_copy(k).wait_send()

    @pl.loop(1, nz)
    def _(k):
        all_copy(k).wait_send()


def deliver(state, totals, state_out, totals_out, sem):
    copy = pltpu.make_async_copy(state, state_out, sem)
    copy.start()
    row = totals[...]
    lane = lax.broadcasted_iota(jnp.int32, row.shape, 1)
    for r in range(ROUNDS):
        totals_out[r] = jnp.sum(jnp.where(lane == r, row, 0.0)).astype(jnp.int32)
    copy.wait()


def per_device(nz, ny, ranks, seeds, flags):
    depth, rows, width = ranks.shape
    f32, i32, vmem, dma = jnp.float32, jnp.int32, pltpu.VMEM, pltpu.SemaphoreType.DMA
    plane = (rows, width)
    scratch = [
        vmem(ranks.shape, f32), vmem(seeds.shape, f32), vmem(flags.shape, i32),
        vmem(ranks.shape, i32), vmem((depth + 2, *plane), f32), vmem((depth + 2, *plane), f32), vmem(plane, f32),
        vmem((3, depth, 1, width), f32), vmem((3, depth, 1, width), f32),
        vmem((4, 1, width), f32), vmem((4, 1, width), f32),
        vmem((ROUNDS, depth + 2, *plane), f32), vmem((ROUNDS, depth, *plane), f32), vmem((ROUNDS, 2, *plane), f32),
        vmem((depth + 2, *plane), i32),
        vmem((ROUNDS, 2, 2, depth, 1, width), f32), vmem((ROUNDS, 2, 2, depth, 1, width), f32),
        vmem((ROUNDS, 4, 2, 1, width), f32), vmem((ROUNDS, 4, 2, 1, width), f32),
        vmem((ny, 1, 128), f32), vmem((nz, 1, 128), f32),
        pltpu.SemaphoreType.REGULAR((4,)), dma((3,)), dma((8,)), dma((8,)), dma((ROUNDS, 10)), dma((ROUNDS, 10)),
        dma((ny,)), dma((ny,)), dma((nz,)), dma((nz,)),
    ]
    state, totals = pl.pallas_call(
        functools.partial(kernel, nz, ny),
        out_shape=(vmem(ranks.shape, i32), vmem((1, 128), f32)),
        in_specs=[pl.BlockSpec(memory_space=pl.ANY)] * 3,
        out_specs=(pl.BlockSpec(memory_space=pltpu.VMEM), pl.BlockSpec(memory_space=pltpu.VMEM)),
        scratch_shapes=scratch,
        compiler_params=pltpu.CompilerParams(collective_id=0, has_side_effects=True),
    )(ranks, seeds, flags)
    return pl.pallas_call(
        deliver,
        out_shape=(jax.ShapeDtypeStruct(ranks.shape, i32), jax.ShapeDtypeStruct((ROUNDS,), i32)),
        in_specs=[pl.BlockSpec(memory_space=pltpu.VMEM)] * 2,
        out_specs=(pl.BlockSpec(memory_space=pl.ANY), pl.BlockSpec(memory_space=pltpu.SMEM)),
        scratch_shapes=[dma],
    )(*[pltpu.with_memory_space_constraint(x, pltpu.VMEM) for x in (state, totals)])


def solution(mesh):
    nz, ny = mesh.shape["gz"], mesh.shape["gy"]
    return jax.shard_map(
        functools.partial(per_device, nz, ny), mesh=mesh,
        in_specs=(P("gz", "gy", None), P(None, "gz", "gy", None), P("gz", "gy", None)),
        out_specs=(P("gz", "gy", None), P()), check_vma=False,
    )
```

```python
import functools

import jax
import jax.numpy as jnp
from jax import lax
from jax.experimental import pallas as pl
from jax.experimental.pallas import tpu as pltpu
from jax.sharding import PartitionSpec as P

ROUNDS = 3
MESH = pl.DeviceIdType.MESH
UP_UP, UP_DOWN, DOWN_UP, DOWN_DOWN = (1, 1), (1, -1), (-1, 1), (-1, -1)
DIAGONALS = (UP_UP, UP_DOWN, DOWN_UP, DOWN_DOWN)
DIRECTIONS = ((1, 0), (-1, 0), (0, 1), (0, -1)) + DIAGONALS
NONE = -3.0
LINK_Y, DEP_Y = 1 << 12, 1 << 13


def kernel(
    nz, ny,
    ranks_hbm, seeds_hbm, flags_hbm,
    state_ref, totals_ref,
    ranks, seeds, flags,
    bits, partial, rowmax, below, edge_y_out, edge_y_in, edge_d_out, edge_d_in,
    packed, near, near_halo, newc, row_out, row_in, diag_out, diag_in,
    couple, whole,
    known, load_sem, edge_send, edge_recv, round_send, round_recv, pair_send, pair_recv, all_send, all_recv,
):
    gz, gy = lax.axis_index("gz"), lax.axis_index("gy")
    depth, rows, width = ranks.shape
    top, end = depth - 1, rows - 1

    loads = [
        pltpu.make_async_copy(seeds_hbm, seeds, load_sem.at[0]),
        pltpu.make_async_copy(ranks_hbm, ranks, load_sem.at[1]),
        pltpu.make_async_copy(flags_hbm, flags, load_sem.at[2]),
    ]
    for load in loads:
        load.start()

    def exists(dz, dy):
        here = None
        for at, step, count in ((gz, dz, nz), (gy, dy, ny)):
            if step:
                inside = at < count - 1 if step > 0 else at > 0
                here = inside if here is None else here & inside
        return here

    there = {d: exists(*d) for d in DIRECTIONS}
    target = {d: (gz + d[0], gy + d[1]) for d in DIRECTIONS}

    barrier = pltpu.get_barrier_semaphore()
    for d in DIAGONALS:
        @pl.when(there[d])
        def _(d=d):
            pl.semaphore_signal(barrier, inc=1, device_id=target[d], device_id_type=MESH)

    for step in (1, nz - 1):
        pl.semaphore_signal(barrier, inc=1, device_id=(lax.rem(gz + step, nz), gy), device_id_type=MESH)

    @pl.loop(1, ny)
    def _(k):
        pl.semaphore_signal(barrier, inc=1, device_id=(gz, lax.rem(gy + k, ny)), device_id_type=MESH)

    strides, reach = [], 1
    while 2 * reach - 1 < nz:
        strides.append(reach)
        reach *= 2

    def tell(i):
        if i < len(strides):
            for step in (strides[i], nz - strides[i]):
                pl.semaphore_signal(known.at[i], inc=1, device_id=(lax.rem(gz + step, nz), gy), device_id_type=MESH)

    def told(i):
        if i < len(strides):
            pl.semaphore_wait(known.at[i], 2)

    def one(flag):
        return jnp.where(flag, 1, 0).astype(jnp.int32)

    sides_z = one(there[(1, 0)]) + one(there[(-1, 0)])
    sides_y = one(there[(0, 1)]) + one(there[(0, -1)])

    started = []

    def remote(direction, source, target_ref, send, recv):
        copy = pltpu.make_async_remote_copy(
            src_ref=source, dst_ref=target_ref, send_sem=send, recv_sem=recv,
            device_id=target[direction], device_id_type=MESH,
        )

        @pl.when(there[direction])
        def _():
            copy.start()

        started.append((direction, copy))
        return direction, copy

    def arrived(pair):
        (dz, dy), copy = pair

        @pl.when(there[(-dz, -dy)])
        def _():
            copy.wait_recv()

    xpos = lax.broadcasted_iota(jnp.int32, (rows, width), 1)
    ypos = lax.broadcasted_iota(jnp.int32, (rows, width), 0)
    first, last = ypos == 0, ypos == end

    def over(row, where, plane):
        return jnp.where(where, jnp.broadcast_to(row, plane.shape), plane)

    def east(plane):
        return pltpu.roll(plane, width - 1, 1)

    def west(plane):
        return pltpu.roll(plane, 1, 1)

    def north(plane):
        return pltpu.roll(plane, rows - 1, 0)

    def south(plane):
        return pltpu.roll(plane, 1, 0)

    zero = jnp.zeros((rows, width), jnp.float32)

    loads[0].wait()

    def in_plane(z):
        c0 = jnp.where(xpos < width - 1, seeds[0, z], 0.0)
        c2 = jnp.where(last & (gy == ny - 1), 0.0, seeds[1, z])
        c4 = seeds[2, z]
        c4 = jnp.where((gz == nz - 1) & (z == top), zero, c4)
        return c0, c2, c4

    def part(z):
        c0, c2, c4 = in_plane(z)
        m = jnp.maximum(jnp.maximum(c0, west(c0)), jnp.maximum(c2, c4))
        m = jnp.maximum(m, jnp.where(first, 0.0, south(c2)))
        if not isinstance(z, int) or z > 0:
            m = jnp.maximum(m, seeds[2, z - 1])
        partial[z + 1] = m
        edge_y_out[0, z] = seeds[1, z, end:rows, :]
        edge_y_out[1, z] = m[end:rows]
        edge_y_out[2, z] = m[0:1]

    part(top)
    part(0)
    edge_d_out[0] = seeds[1, top, end:rows, :]
    edge_d_out[1] = seeds[2, top, end:rows, :]
    edge_d_out[2] = seeds[2, top, 0:1, :]
    edge_d_out[3] = seeds[1, 0, end:rows, :]

    pl.semaphore_wait(barrier, 2 + ny - 1 + sides_z * sides_y)

    def edge(direction, source, target_ref, i):
        return remote(direction, source, target_ref, edge_send.at[i], edge_recv.at[i])

    edge_d = [
        edge(UP_UP, edge_d_out.at[0:2], edge_d_in.at[0:2], 0),
        edge(UP_DOWN, edge_d_out.at[2:3], edge_d_in.at[2:3], 1),
        edge(DOWN_UP, edge_d_out.at[3:4], edge_d_in.at[3:4], 2),
    ]
    edge_z = [
        edge((1, 0), seeds.at[2, top], below, 3),
        edge((1, 0), partial.at[depth], partial.at[0], 4),
        edge((-1, 0), partial.at[1], partial.at[depth + 1], 5),
    ]
    tell(0)
    for z in range(1, top):
        part(z)
    edge_y = [
        edge((0, 1), edge_y_out.at[0:2], edge_y_in.at[0:2], 6),
        edge((0, -1), edge_y_out.at[2:3], edge_y_in.at[2:3], 7),
    ]

    def fill(direction, *refs_values):
        @pl.when(jnp.logical_not(there[direction]))
        def _():
            for ref, value in refs_values:
                ref[...] = jnp.full(ref.shape, value, ref.dtype)

    fill((-1, 0), (below, 0.0), (partial.at[0], 0.0), *[(packed.at[r, 0], NONE) for r in range(ROUNDS)],
         *[(near_halo.at[r, 0], NONE) for r in range(ROUNDS)])
    fill((1, 0), (partial.at[depth + 1], 0.0), *[(packed.at[r, depth + 1], NONE) for r in range(ROUNDS)],
         *[(near_halo.at[r, 1], NONE) for r in range(ROUNDS)])
    fill((0, -1), (edge_y_in.at[0:2], 0.0), *[(row_in.at[r, 0], NONE) for r in range(ROUNDS)])
    fill((0, 1), (edge_y_in.at[2:3], 0.0), *[(row_in.at[r, 1], NONE) for r in range(ROUNDS)])
    fill(DOWN_DOWN, (edge_d_in.at[0:2], 0.0))
    fill(DOWN_UP, (edge_d_in.at[2:3], 0.0))
    fill(UP_DOWN, (edge_d_in.at[3:4], 0.0))
    for i, d in enumerate(DIAGONALS):
        fill((-d[0], -d[1]), *[(diag_in.at[r, i], NONE) for r in range(ROUNDS)])

    def whole_rowmax(z):
        m = jnp.maximum(partial[z + 1], jnp.where(first, jnp.broadcast_to(edge_y_in[0, z], zero.shape), 0.0))
        if z == 0:
            m = jnp.maximum(m, below[...])
        rowmax[z + 1] = m

    def outside_rowmax():
        m = partial[0]
        rowmax[0] = jnp.maximum(m, jnp.where(first, jnp.broadcast_to(edge_d_in[0], zero.shape), 0.0))
        m = jnp.maximum(partial[depth + 1], in_plane(top)[2])
        rowmax[depth + 1] = jnp.maximum(m, jnp.where(first, jnp.broadcast_to(edge_d_in[3], zero.shape), 0.0))

    def strengths(z):
        c0, c2, c4 = in_plane(z)
        c1 = west(c0)
        c3 = over(edge_y_in[0, z], first, south(c2))
        c5 = below[...] if z == 0 else seeds[2, z - 1]
        mine = rowmax[z + 1]
        low = edge_y_in[1, z]
        high = jnp.maximum(edge_y_in[2, z], c2[end:rows])
        if z == 0:
            low = jnp.maximum(low, edge_d_in[1])
            high = jnp.maximum(high, edge_d_in[2])
        others = [
            east(mine), west(mine), over(high, last, north(mine)), over(low, first, south(mine)),
            rowmax[z + 2], rowmax[z],
        ]
        word = jnp.zeros((rows, width), jnp.int32)
        measure = ranks[z]
        outer_link = outer_dep = None
        for d, (cost, other) in enumerate(zip((c0, c1, c2, c3, c4, c5), others)):
            twice = 2.0 * cost
            depends = (cost > 0) & (twice >= mine)
            feeds = (cost > 0) & (twice >= other)
            measure = jnp.where(feeds, 2.0 * measure, measure)
            link = depends | feeds
            if d in (2, 3):
                border = last if d == 2 else first
                outer = jnp.where(link & border, LINK_Y, 0) + jnp.where(depends & border, DEP_Y, 0)
                word = word + outer
                link = link & jnp.logical_not(border)
                depends = depends & jnp.logical_not(border)
            word = word + jnp.where(link, 1 << d, 0) + jnp.where(depends, 1 << (d + 6), 0)
        bits[z] = word
        flag = flags[z]
        packed[0, z + 1] = jnp.where(flag == 0, measure, jnp.where(flag == 2, -2.0, -1.0))

    def linked(word, mask, value):
        return jnp.where((word & mask) != 0, value, NONE)

    def near_inside(r, z):
        word, here = bits[z], packed[r, z + 1]
        m = jnp.maximum(linked(word, 1, east(here)), linked(word, 2, west(here)))
        m = jnp.maximum(m, linked(word, 4, north(here)))
        m = jnp.maximum(m, linked(word, 8, south(here)))
        if z < top:
            m = jnp.maximum(m, linked(word, 16, packed[r, z + 2]))
        if z > 0:
            m = jnp.maximum(m, linked(word, 32, packed[r, z]))
        near[r, z] = m
        for arr, plane in ((0, here), (1, m)):
            row_out[r, 0, arr, z] = plane[end:rows]
            row_out[r, 1, arr, z] = plane[0:1]

    def corner(r, i, d):
        z, row, z_mask = (top if d[0] > 0 else 0), (end if d[1] > 0 else 0), (16 if d[0] > 0 else 32)
        word, value = bits[z, row : row + 1, :], packed[r, z + 1, row : row + 1, :]
        diag_out[r, i, 0] = linked(word, LINK_Y, value)
        diag_out[r, i, 1] = linked(word, z_mask, value)

    def send_packed(r):
        send, recv = round_send.at[r], round_recv.at[r]
        for i, d in enumerate(DIAGONALS):
            corner(r, i, d)
        return [
            *[remote(d, diag_out.at[r, i], diag_in.at[r, i], send.at[6 + i], recv.at[6 + i]) for i, d in enumerate(DIAGONALS)],
            remote((1, 0), packed.at[r, depth], packed.at[r, 0], send.at[0], recv.at[0]),
            remote((-1, 0), packed.at[r, 1], packed.at[r, depth + 1], send.at[2], recv.at[2]),
        ]

    def send_near(r):
        send, recv = round_send.at[r], round_recv.at[r]
        return [
            remote((1, 0), near.at[r, top], near_halo.at[r, 0], send.at[1], recv.at[1]),
            remote((-1, 0), near.at[r, 0], near_halo.at[r, 1], send.at[3], recv.at[3]),
        ]

    def send_rows(r):
        send, recv = round_send.at[r], round_recv.at[r]
        return [
            remote((0, 1), row_out.at[r, 0], row_in.at[r, 0], send.at[4], recv.at[4]),
            remote((0, -1), row_out.at[r, 1], row_in.at[r, 1], send.at[5], recv.at[5]),
        ]

    def yes(mask):
        return jnp.where(mask, -1, 0).astype(jnp.int32)

    def halo_rows(r, arr, z):
        low = jnp.broadcast_to(row_in[r, 0, arr, z], (rows, width))
        return over(row_in[r, 1, arr, z], last, low)

    def finish_near(r, z):
        word, here = bits[z], packed[r, z + 1]
        m = jnp.maximum(near[r, z], linked(word, LINK_Y, halo_rows(r, 0, z)))
        if z == top:
            m = jnp.maximum(m, linked(word, 16, packed[r, z + 2]))
        if z == 0:
            m = jnp.maximum(m, linked(word, 32, packed[r, z]))
        newc[z + 1] = yes((here >= 0) & (here > m))

    def outside_z(r, low):
        z, at, mask = (0, 0, 32) if low else (top, depth + 1, 16)
        there_packed, mine = packed[r, at], packed[r, z + 1]
        limit = jnp.maximum(near_halo[r, 0 if low else 1], linked(bits[z], mask, mine))
        i, j = (0, 1) if low else (2, 3)
        limit = jnp.where(first, jnp.maximum(limit, jnp.broadcast_to(diag_in[r, i, 0], limit.shape)), limit)
        limit = jnp.where(last, jnp.maximum(limit, jnp.broadcast_to(diag_in[r, j, 0], limit.shape)), limit)
        newc[at] = yes((there_packed >= 0) & (there_packed > limit))

    def update(r, z, count):
        word, here, chosen = bits[z], packed[r, z + 1], newc[z + 1]
        outer, limit = halo_rows(r, 0, z), halo_rows(r, 1, z)
        limit = jnp.maximum(limit, linked(word, LINK_Y, here))
        if z in (0, top):
            i, j = (0, 1) if z == 0 else (2, 3)
            corner_value = over(diag_in[r, j, 1], last, jnp.broadcast_to(diag_in[r, i, 1], (rows, width)))
            limit = jnp.maximum(limit, corner_value)
        hit = word & DEP_Y & yes((outer >= 0) & (outer > limit))
        for d, value in enumerate((east(chosen), west(chosen), north(chosen), south(chosen), newc[z + 2], newc[z])):
            hit = hit | (word & (1 << (d + 6)) & value)
        after = jnp.where(chosen != 0, -2.0, jnp.where((here >= 0) & (hit != 0), -1.0, here))
        if r + 1 < ROUNDS:
            packed[r + 1, z + 1] = after
        else:
            state_ref[z] = jnp.where(after >= 0, 0, jnp.where(after == -2.0, 2, 1)).astype(jnp.int32)
        return count + jnp.where(after >= 0, 1.0, 0.0)

    def wait_all(pairs):
        for pair in pairs:
            arrived(pair)

    inner, middle = range(1, top), range(2, top - 1)
    loads[1].wait()
    loads[2].wait()
    wait_all(edge_y)
    for z in inner:
        whole_rowmax(z)
    for z in middle:
        strengths(z)
    wait_all(edge_z)
    wait_all(edge_d)
    whole_rowmax(0)
    whole_rowmax(top)
    outside_rowmax()
    strengths(0)
    strengths(top)
    told(0)
    tell(1)

    lane = lax.broadcasted_iota(jnp.int32, (1, 128), 1)
    counted = jnp.zeros((1, 128), jnp.float32)
    for r in range(ROUNDS):
        sent_packed = send_packed(r)
        if r == 0:
            strengths(1)
            strengths(top - 1)
        near_inside(r, 0)
        near_inside(r, top)
        sent_near = send_near(r)
        for z in inner:
            near_inside(r, z)
        sent_rows = send_rows(r)

        wait_all(sent_rows)
        if r == ROUNDS - 1:
            told(r + 1)
            tell(r + 2)
        for z in inner:
            finish_near(r, z)
        count = zero
        for z in middle:
            count = update(r, z, count)
        wait_all(sent_packed)
        finish_near(r, 0)
        finish_near(r, top)
        count = update(r, 1, count)
        count = update(r, top - 1, count)
        wait_all(sent_near)
        outside_z(r, True)
        outside_z(r, False)
        count = update(r, 0, count)
        count = update(r, top, count)
        if r < ROUNDS - 1:
            told(r + 1)
            tell(r + 2)
        counted = jnp.where(lane == r, jnp.sum(count), counted)

    half = ny // 2
    lone, core = gz * half + gy // 2, lax.rem(gy, 2)
    couple[core] = counted
    to_partner = pltpu.make_async_remote_copy(
        src_ref=couple.at[core], dst_ref=couple.at[core], send_sem=pair_send, recv_sem=pair_recv,
        device_id=(gz, gy + 1 - 2 * core), device_id_type=MESH)
    to_partner.start()
    to_partner.wait_recv()
    told(ROUNDS + 1)
    whole[lone] = couple[0] + couple[1]

    def all_copy(kz, ky):
        return pltpu.make_async_remote_copy(
            src_ref=whole.at[lone], dst_ref=whole.at[lone], send_sem=all_send, recv_sem=all_recv,
            device_id=(lax.rem(gz + kz, nz), lax.rem(gy + 2 * ky, ny)), device_id_type=MESH)

    @pl.loop(0, nz)
    def _(i):
        kz = lax.rem(i + 4, nz)
        for ky in range(1, half):
            all_copy(kz, ky).start()

        @pl.when(kz > 0)
        def _():
            all_copy(kz, 0).start()

    others = whole.at[0 : nz * half - 1]
    pltpu.make_async_copy(others, others, all_recv).wait()
    totals_ref[...] = jnp.sum(whole[...], axis=0)
    pltpu.make_async_copy(others, others, all_send).wait()
    to_partner.wait_send()

    for (dz, dy), copy in started:
        @pl.when(there[(dz, dy)])
        def _(copy=copy):
            copy.wait_send()


def deliver(state, totals, state_out, totals_out, sem):
    copy = pltpu.make_async_copy(state, state_out, sem)
    copy.start()
    row = totals[...]
    lane = lax.broadcasted_iota(jnp.int32, row.shape, 1)
    for r in range(ROUNDS):
        totals_out[r] = jnp.sum(jnp.where(lane == r, row, 0.0)).astype(jnp.int32)
    copy.wait()


def per_device(nz, ny, ranks, seeds, flags):
    depth, rows, width = ranks.shape
    f32, i32, vmem, dma = jnp.float32, jnp.int32, pltpu.VMEM, pltpu.SemaphoreType.DMA
    plane = (rows, width)
    scratch = [
        vmem(ranks.shape, f32), vmem(seeds.shape, f32), vmem(flags.shape, i32),
        vmem(ranks.shape, i32), vmem((depth + 2, *plane), f32), vmem((depth + 2, *plane), f32), vmem(plane, f32),
        vmem((3, depth, 1, width), f32), vmem((3, depth, 1, width), f32),
        vmem((4, 1, width), f32), vmem((4, 1, width), f32),
        vmem((ROUNDS, depth + 2, *plane), f32), vmem((ROUNDS, depth, *plane), f32), vmem((ROUNDS, 2, *plane), f32),
        vmem((depth + 2, *plane), i32),
        vmem((ROUNDS, 2, 2, depth, 1, width), f32), vmem((ROUNDS, 2, 2, depth, 1, width), f32),
        vmem((ROUNDS, 4, 2, 1, width), f32), vmem((ROUNDS, 4, 2, 1, width), f32),
        vmem((2, 1, 128), f32), vmem((nz * ny // 2, 1, 128), f32),
        pltpu.SemaphoreType.REGULAR((ROUNDS + 2,)), dma((3,)), dma((8,)), dma((8,)), dma((ROUNDS, 10)), dma((ROUNDS, 10)),
        dma, dma, dma, dma,
    ]
    state, totals = pl.pallas_call(
        functools.partial(kernel, nz, ny),
        out_shape=(vmem(ranks.shape, i32), vmem((1, 128), f32)),
        in_specs=[pl.BlockSpec(memory_space=pl.ANY)] * 3,
        out_specs=(pl.BlockSpec(memory_space=pltpu.VMEM), pl.BlockSpec(memory_space=pltpu.VMEM)),
        scratch_shapes=scratch,
        compiler_params=pltpu.CompilerParams(collective_id=0, has_side_effects=True),
    )(ranks, seeds, flags)
    return pl.pallas_call(
        deliver,
        out_shape=(jax.ShapeDtypeStruct(ranks.shape, i32), jax.ShapeDtypeStruct((ROUNDS,), i32)),
        in_specs=[pl.BlockSpec(memory_space=pltpu.VMEM)] * 2,
        out_specs=(pl.BlockSpec(memory_space=pl.ANY), pl.BlockSpec(memory_space=pltpu.SMEM)),
        scratch_shapes=[dma],
    )(*[pltpu.with_memory_space_constraint(x, pltpu.VMEM) for x in (state, totals)])


def solution(mesh):
    nz, ny = mesh.shape["gz"], mesh.shape["gy"]
    return jax.shard_map(
        functools.partial(per_device, nz, ny), mesh=mesh,
        in_specs=(P("gz", "gy", None), P(None, "gz", "gy", None), P("gz", "gy", None)),
        out_specs=(P("gz", "gy", None), P()), check_vma=False,
    )
```

```python
import functools

import jax
import jax.numpy as jnp
from jax import lax
from jax.experimental import pallas as pl
from jax.experimental.pallas import tpu as pltpu
from jax.sharding import PartitionSpec as P

ROUNDS = 3
EARLY = 1
MESH = pl.DeviceIdType.MESH
UP_UP, UP_DOWN, DOWN_UP, DOWN_DOWN = (1, 1), (1, -1), (-1, 1), (-1, -1)
DIAGONALS = (UP_UP, UP_DOWN, DOWN_UP, DOWN_DOWN)
DIRECTIONS = ((1, 0), (-1, 0), (0, 1), (0, -1)) + DIAGONALS
NONE = -3.0
LINK_Y, DEP_Y = 1 << 12, 1 << 13


def kernel(
    nz, ny,
    ranks_hbm, seeds_hbm, flags_hbm,
    state_ref, totals_ref,
    ranks, seeds, flags,
    bits, partial, rowmax, below, edge_y_out, edge_y_in, edge_d_out, edge_d_in,
    packed, near, near_halo, newc, row_out, row_in, diag_out, diag_in,
    couple, single, whole,
    known, load_sem, edge_send, edge_recv, round_send, round_recv, pair_send, pair_recv, one_send, one_recv, all_send, all_recv,
):
    gz, gy = lax.axis_index("gz"), lax.axis_index("gy")
    depth, rows, width = ranks.shape
    top, end = depth - 1, rows - 1

    loads = [
        pltpu.make_async_copy(seeds_hbm, seeds, load_sem.at[0]),
        pltpu.make_async_copy(ranks_hbm, ranks, load_sem.at[1]),
        pltpu.make_async_copy(flags_hbm, flags, load_sem.at[2]),
    ]
    for load in loads:
        load.start()

    def exists(dz, dy):
        here = None
        for at, step, count in ((gz, dz, nz), (gy, dy, ny)):
            if step:
                inside = at < count - 1 if step > 0 else at > 0
                here = inside if here is None else here & inside
        return here

    there = {d: exists(*d) for d in DIRECTIONS}
    target = {d: (gz + d[0], gy + d[1]) for d in DIRECTIONS}

    barrier = pltpu.get_barrier_semaphore()
    for d in DIAGONALS:
        @pl.when(there[d])
        def _(d=d):
            pl.semaphore_signal(barrier, inc=1, device_id=target[d], device_id_type=MESH)

    for step in (1, nz - 1):
        pl.semaphore_signal(barrier, inc=1, device_id=(lax.rem(gz + step, nz), gy), device_id_type=MESH)

    @pl.loop(1, ny)
    def _(k):
        pl.semaphore_signal(barrier, inc=1, device_id=(gz, lax.rem(gy + k, ny)), device_id_type=MESH)

    strides, reach = [], 1
    while 2 * reach - 1 < nz:
        strides.append(reach)
        reach *= 2

    def tell(i):
        if i < len(strides):
            for step in (strides[i], nz - strides[i]):
                pl.semaphore_signal(known.at[i], inc=1, device_id=(lax.rem(gz + step, nz), gy), device_id_type=MESH)

    def told(i):
        if i < len(strides):
            pl.semaphore_wait(known.at[i], 2)

    def one(flag):
        return jnp.where(flag, 1, 0).astype(jnp.int32)

    sides_z = one(there[(1, 0)]) + one(there[(-1, 0)])
    sides_y = one(there[(0, 1)]) + one(there[(0, -1)])

    started = []

    def remote(direction, source, target_ref, send, recv):
        copy = pltpu.make_async_remote_copy(
            src_ref=source, dst_ref=target_ref, send_sem=send, recv_sem=recv,
            device_id=target[direction], device_id_type=MESH,
        )

        @pl.when(there[direction])
        def _():
            copy.start()

        started.append((direction, copy))
        return direction, copy

    def arrived(pair):
        (dz, dy), copy = pair

        @pl.when(there[(-dz, -dy)])
        def _():
            copy.wait_recv()

    xpos = lax.broadcasted_iota(jnp.int32, (rows, width), 1)
    ypos = lax.broadcasted_iota(jnp.int32, (rows, width), 0)
    first, last = ypos == 0, ypos == end

    def over(row, where, plane):
        return jnp.where(where, jnp.broadcast_to(row, plane.shape), plane)

    def east(plane):
        return pltpu.roll(plane, width - 1, 1)

    def west(plane):
        return pltpu.roll(plane, 1, 1)

    def north(plane):
        return pltpu.roll(plane, rows - 1, 0)

    def south(plane):
        return pltpu.roll(plane, 1, 0)

    zero = jnp.zeros((rows, width), jnp.float32)

    loads[0].wait()

    def in_plane(z):
        c0 = jnp.where(xpos < width - 1, seeds[0, z], 0.0)
        c2 = jnp.where(last & (gy == ny - 1), 0.0, seeds[1, z])
        c4 = seeds[2, z]
        c4 = jnp.where((gz == nz - 1) & (z == top), zero, c4)
        return c0, c2, c4

    def part(z):
        c0, c2, c4 = in_plane(z)
        m = jnp.maximum(jnp.maximum(c0, west(c0)), jnp.maximum(c2, c4))
        m = jnp.maximum(m, jnp.where(first, 0.0, south(c2)))
        if not isinstance(z, int) or z > 0:
            m = jnp.maximum(m, seeds[2, z - 1])
        partial[z + 1] = m
        edge_y_out[0, z] = seeds[1, z, end:rows, :]
        edge_y_out[1, z] = m[end:rows]
        edge_y_out[2, z] = m[0:1]

    part(top)
    part(0)
    edge_d_out[0] = seeds[1, top, end:rows, :]
    edge_d_out[1] = seeds[2, top, end:rows, :]
    edge_d_out[2] = seeds[2, top, 0:1, :]
    edge_d_out[3] = seeds[1, 0, end:rows, :]

    pl.semaphore_wait(barrier, 2 + ny - 1 + sides_z * sides_y)

    def edge(direction, source, target_ref, i):
        return remote(direction, source, target_ref, edge_send.at[i], edge_recv.at[i])

    edge_d = [
        edge(UP_UP, edge_d_out.at[0:2], edge_d_in.at[0:2], 0),
        edge(UP_DOWN, edge_d_out.at[2:3], edge_d_in.at[2:3], 1),
        edge(DOWN_UP, edge_d_out.at[3:4], edge_d_in.at[3:4], 2),
    ]
    edge_z = [
        edge((1, 0), seeds.at[2, top], below, 3),
        edge((1, 0), partial.at[depth], partial.at[0], 4),
        edge((-1, 0), partial.at[1], partial.at[depth + 1], 5),
    ]
    tell(0)
    for z in range(1, top):
        part(z)
    edge_y = [
        edge((0, 1), edge_y_out.at[0:2], edge_y_in.at[0:2], 6),
        edge((0, -1), edge_y_out.at[2:3], edge_y_in.at[2:3], 7),
    ]

    def fill(direction, *refs_values):
        @pl.when(jnp.logical_not(there[direction]))
        def _():
            for ref, value in refs_values:
                ref[...] = jnp.full(ref.shape, value, ref.dtype)

    fill((-1, 0), (below, 0.0), (partial.at[0], 0.0), *[(packed.at[r, 0], NONE) for r in range(ROUNDS)],
         *[(near_halo.at[r, 0], NONE) for r in range(ROUNDS)])
    fill((1, 0), (partial.at[depth + 1], 0.0), *[(packed.at[r, depth + 1], NONE) for r in range(ROUNDS)],
         *[(near_halo.at[r, 1], NONE) for r in range(ROUNDS)])
    fill((0, -1), (edge_y_in.at[0:2], 0.0), *[(row_in.at[r, 0], NONE) for r in range(ROUNDS)])
    fill((0, 1), (edge_y_in.at[2:3], 0.0), *[(row_in.at[r, 1], NONE) for r in range(ROUNDS)])
    fill(DOWN_DOWN, (edge_d_in.at[0:2], 0.0))
    fill(DOWN_UP, (edge_d_in.at[2:3], 0.0))
    fill(UP_DOWN, (edge_d_in.at[3:4], 0.0))
    for i, d in enumerate(DIAGONALS):
        fill((-d[0], -d[1]), *[(diag_in.at[r, i], NONE) for r in range(ROUNDS)])

    def whole_rowmax(z):
        m = jnp.maximum(partial[z + 1], jnp.where(first, jnp.broadcast_to(edge_y_in[0, z], zero.shape), 0.0))
        if z == 0:
            m = jnp.maximum(m, below[...])
        rowmax[z + 1] = m

    def outside_rowmax():
        m = partial[0]
        rowmax[0] = jnp.maximum(m, jnp.where(first, jnp.broadcast_to(edge_d_in[0], zero.shape), 0.0))
        m = jnp.maximum(partial[depth + 1], in_plane(top)[2])
        rowmax[depth + 1] = jnp.maximum(m, jnp.where(first, jnp.broadcast_to(edge_d_in[3], zero.shape), 0.0))

    def strengths(z):
        c0, c2, c4 = in_plane(z)
        c1 = west(c0)
        c3 = over(edge_y_in[0, z], first, south(c2))
        c5 = below[...] if z == 0 else seeds[2, z - 1]
        mine = rowmax[z + 1]
        low = edge_y_in[1, z]
        high = jnp.maximum(edge_y_in[2, z], c2[end:rows])
        if z == 0:
            low = jnp.maximum(low, edge_d_in[1])
            high = jnp.maximum(high, edge_d_in[2])
        others = [
            east(mine), west(mine), over(high, last, north(mine)), over(low, first, south(mine)),
            rowmax[z + 2], rowmax[z],
        ]
        word = jnp.zeros((rows, width), jnp.int32)
        measure = ranks[z]
        outer_link = outer_dep = None
        for d, (cost, other) in enumerate(zip((c0, c1, c2, c3, c4, c5), others)):
            twice = 2.0 * cost
            depends = (cost > 0) & (twice >= mine)
            feeds = (cost > 0) & (twice >= other)
            measure = jnp.where(feeds, 2.0 * measure, measure)
            link = depends | feeds
            if d in (2, 3):
                border = last if d == 2 else first
                outer = jnp.where(link & border, LINK_Y, 0) + jnp.where(depends & border, DEP_Y, 0)
                word = word + outer
                link = link & jnp.logical_not(border)
                depends = depends & jnp.logical_not(border)
            word = word + jnp.where(link, 1 << d, 0) + jnp.where(depends, 1 << (d + 6), 0)
        bits[z] = word
        flag = flags[z]
        packed[0, z + 1] = jnp.where(flag == 0, measure, jnp.where(flag == 2, -2.0, -1.0))

    def linked(word, mask, value):
        return jnp.where((word & mask) != 0, value, NONE)

    def near_inside(r, z):
        word, here = bits[z], packed[r, z + 1]
        m = jnp.maximum(linked(word, 1, east(here)), linked(word, 2, west(here)))
        m = jnp.maximum(m, linked(word, 4, north(here)))
        m = jnp.maximum(m, linked(word, 8, south(here)))
        if z < top:
            m = jnp.maximum(m, linked(word, 16, packed[r, z + 2]))
        if z > 0:
            m = jnp.maximum(m, linked(word, 32, packed[r, z]))
        near[r, z] = m
        for arr, plane in ((0, here), (1, m)):
            row_out[r, 0, arr, z] = plane[end:rows]
            row_out[r, 1, arr, z] = plane[0:1]

    def corner(r, i, d):
        z, row, z_mask = (top if d[0] > 0 else 0), (end if d[1] > 0 else 0), (16 if d[0] > 0 else 32)
        word, value = bits[z, row : row + 1, :], packed[r, z + 1, row : row + 1, :]
        diag_out[r, i, 0] = linked(word, LINK_Y, value)
        diag_out[r, i, 1] = linked(word, z_mask, value)

    def send_packed(r):
        send, recv = round_send.at[r], round_recv.at[r]
        for i, d in enumerate(DIAGONALS):
            corner(r, i, d)
        return [
            *[remote(d, diag_out.at[r, i], diag_in.at[r, i], send.at[6 + i], recv.at[6 + i]) for i, d in enumerate(DIAGONALS)],
            remote((1, 0), packed.at[r, depth], packed.at[r, 0], send.at[0], recv.at[0]),
            remote((-1, 0), packed.at[r, 1], packed.at[r, depth + 1], send.at[2], recv.at[2]),
        ]

    def send_near(r):
        send, recv = round_send.at[r], round_recv.at[r]
        return [
            remote((1, 0), near.at[r, top], near_halo.at[r, 0], send.at[1], recv.at[1]),
            remote((-1, 0), near.at[r, 0], near_halo.at[r, 1], send.at[3], recv.at[3]),
        ]

    def send_rows(r):
        send, recv = round_send.at[r], round_recv.at[r]
        return [
            remote((0, 1), row_out.at[r, 0], row_in.at[r, 0], send.at[4], recv.at[4]),
            remote((0, -1), row_out.at[r, 1], row_in.at[r, 1], send.at[5], recv.at[5]),
        ]

    def yes(mask):
        return jnp.where(mask, -1, 0).astype(jnp.int32)

    def halo_rows(r, arr, z):
        low = jnp.broadcast_to(row_in[r, 0, arr, z], (rows, width))
        return over(row_in[r, 1, arr, z], last, low)

    def finish_near(r, z):
        word, here = bits[z], packed[r, z + 1]
        m = jnp.maximum(near[r, z], linked(word, LINK_Y, halo_rows(r, 0, z)))
        if z == top:
            m = jnp.maximum(m, linked(word, 16, packed[r, z + 2]))
        if z == 0:
            m = jnp.maximum(m, linked(word, 32, packed[r, z]))
        newc[z + 1] = yes((here >= 0) & (here > m))

    def outside_z(r, low):
        z, at, mask = (0, 0, 32) if low else (top, depth + 1, 16)
        there_packed, mine = packed[r, at], packed[r, z + 1]
        limit = jnp.maximum(near_halo[r, 0 if low else 1], linked(bits[z], mask, mine))
        i, j = (0, 1) if low else (2, 3)
        limit = jnp.where(first, jnp.maximum(limit, jnp.broadcast_to(diag_in[r, i, 0], limit.shape)), limit)
        limit = jnp.where(last, jnp.maximum(limit, jnp.broadcast_to(diag_in[r, j, 0], limit.shape)), limit)
        newc[at] = yes((there_packed >= 0) & (there_packed > limit))

    def update(r, z, count):
        word, here, chosen = bits[z], packed[r, z + 1], newc[z + 1]
        outer, limit = halo_rows(r, 0, z), halo_rows(r, 1, z)
        limit = jnp.maximum(limit, linked(word, LINK_Y, here))
        if z in (0, top):
            i, j = (0, 1) if z == 0 else (2, 3)
            corner_value = over(diag_in[r, j, 1], last, jnp.broadcast_to(diag_in[r, i, 1], (rows, width)))
            limit = jnp.maximum(limit, corner_value)
        hit = word & DEP_Y & yes((outer >= 0) & (outer > limit))
        for d, value in enumerate((east(chosen), west(chosen), north(chosen), south(chosen), newc[z + 2], newc[z])):
            hit = hit | (word & (1 << (d + 6)) & value)
        after = jnp.where(chosen != 0, -2.0, jnp.where((here >= 0) & (hit != 0), -1.0, here))
        if r + 1 < ROUNDS:
            packed[r + 1, z + 1] = after
        else:
            state_ref[z] = jnp.where(after >= 0, 0, jnp.where(after == -2.0, 2, 1)).astype(jnp.int32)
        return count + jnp.where(after >= 0, 1.0, 0.0)

    def wait_all(pairs):
        for pair in pairs:
            arrived(pair)

    inner, middle = range(1, top), range(2, top - 1)
    loads[1].wait()
    loads[2].wait()
    wait_all(edge_y)
    for z in inner:
        whole_rowmax(z)
    for z in middle:
        strengths(z)
    wait_all(edge_z)
    wait_all(edge_d)
    whole_rowmax(0)
    whole_rowmax(top)
    outside_rowmax()
    strengths(0)
    strengths(top)

    lane = lax.broadcasted_iota(jnp.int32, (1, 128), 1)
    counted = jnp.zeros((1, 128), jnp.float32)

    def with_count(r):
        total = jnp.sum(jnp.sum(count, axis=0, keepdims=True), axis=1, keepdims=True)
        return jnp.where(lane == r, jnp.broadcast_to(total, counted.shape), counted)

    for r in range(ROUNDS):
        sent_packed = send_packed(r)
        if r == 0:
            strengths(1)
            strengths(top - 1)
        near_inside(r, 0)
        near_inside(r, top)
        sent_near = send_near(r)
        for z in inner:
            near_inside(r, z)
        sent_rows = send_rows(r)
        if r:
            counted = with_count(r - 1)
        told(r)
        tell(r + 1)

        wait_all(sent_rows)
        if r == ROUNDS - 1:
            told(r + 1)
            tell(r + 2)
        for z in inner:
            finish_near(r, z)
        count = zero
        for z in middle:
            count = update(r, z, count)
        wait_all(sent_packed)
        finish_near(r, 0)
        finish_near(r, top)
        count = update(r, 1, count)
        count = update(r, top - 1, count)
        wait_all(sent_near)
        outside_z(r, True)
        outside_z(r, False)
        count = update(r, 0, count)
        count = update(r, top, count)

    half, devices = ny // 2, nz * ny
    column = 8 if nz % 8 == 0 else nz
    columns, early = nz // column, EARLY if column > EARLY else 1
    chip, core, me = gz * half + gy // 2, lax.rem(gy, 2), gz * ny + gy
    is_early = lax.rem(gz, column) < early
    n_early = columns * early * ny
    counted = with_count(ROUNDS - 1)
    couple[core] = counted
    to_partner = pltpu.make_async_remote_copy(
        src_ref=couple.at[core], dst_ref=couple.at[core], send_sem=pair_send, recv_sem=pair_recv,
        device_id=(gz, gy + 1 - 2 * core), device_id_type=MESH)
    to_partner.start()
    told(ROUNDS + 1)

    def at_place(i):
        return lax.rem(i, columns) * column + i // columns

    @pl.loop(0, columns * early)
    def _(i):
        to_z = at_place(i)
        for to_y in range(ny):
            @pl.when((to_z != gz) | (to_y != gy))
            def _():
                pltpu.make_async_remote_copy(
                    src_ref=couple.at[core], dst_ref=single.at[me], send_sem=one_send, recv_sem=one_recv,
                    device_id=(to_z, to_y), device_id_type=MESH).start()

    to_partner.wait_recv()
    whole[chip] = couple[0] + couple[1]

    @pl.loop(columns * early, nz)
    def _(i):
        to_z = at_place(i)
        for pair in range(half):
            @pl.when((to_z != gz) | (pair != gy // 2))
            def _():
                pltpu.make_async_remote_copy(
                    src_ref=whole.at[chip], dst_ref=whole.at[chip], send_sem=all_send, recv_sem=all_recv,
                    device_id=(to_z, 2 * pair + core), device_id_type=MESH).start()

    def passed(buffer, count, sem):
        part = buffer.at[0:count]
        pltpu.make_async_copy(part, part, sem).wait()

    for (dz, dy), copy in started:
        @pl.when(there[(dz, dy)])
        def _(copy=copy):
            copy.wait_send()
    to_partner.wait_send()

    @pl.when(is_early)
    def _():
        single[me] = counted
        passed(single, n_early - 1, one_send)
        passed(whole, (devices - n_early) // 2, all_send)
        passed(single, devices - 1, one_recv)
        totals_ref[...] = jnp.sum(single[...], axis=0)

    @pl.when(jnp.logical_not(is_early))
    def _():
        passed(single, n_early, one_send)
        passed(whole, (devices - n_early) // 2 - 1, all_send)
        passed(whole, devices // 2 - 1, all_recv)
        totals_ref[...] = jnp.sum(whole[...], axis=0)


def deliver(state, totals, state_out, totals_out, sem):
    copy = pltpu.make_async_copy(state, state_out, sem)
    copy.start()
    row = totals[...]
    lane = lax.broadcasted_iota(jnp.int32, row.shape, 1)
    for r in range(ROUNDS):
        totals_out[r] = jnp.sum(jnp.where(lane == r, row, 0.0)).astype(jnp.int32)
    copy.wait()


def per_device(nz, ny, ranks, seeds, flags):
    depth, rows, width = ranks.shape
    f32, i32, vmem, dma = jnp.float32, jnp.int32, pltpu.VMEM, pltpu.SemaphoreType.DMA
    plane = (rows, width)
    scratch = [
        vmem(ranks.shape, f32), vmem(seeds.shape, f32), vmem(flags.shape, i32),
        vmem(ranks.shape, i32), vmem((depth + 2, *plane), f32), vmem((depth + 2, *plane), f32), vmem(plane, f32),
        vmem((3, depth, 1, width), f32), vmem((3, depth, 1, width), f32),
        vmem((4, 1, width), f32), vmem((4, 1, width), f32),
        vmem((ROUNDS, depth + 2, *plane), f32), vmem((ROUNDS, depth, *plane), f32), vmem((ROUNDS, 2, *plane), f32),
        vmem((depth + 2, *plane), i32),
        vmem((ROUNDS, 2, 2, depth, 1, width), f32), vmem((ROUNDS, 2, 2, depth, 1, width), f32),
        vmem((ROUNDS, 4, 2, 1, width), f32), vmem((ROUNDS, 4, 2, 1, width), f32),
        vmem((2, 1, 128), f32), vmem((nz * ny, 1, 128), f32), vmem((nz * ny // 2, 1, 128), f32),
        pltpu.SemaphoreType.REGULAR((ROUNDS + 2,)), dma((3,)), dma((8,)), dma((8,)), dma((ROUNDS, 10)), dma((ROUNDS, 10)),
        dma, dma, dma, dma, dma, dma,
    ]
    state, totals = pl.pallas_call(
        functools.partial(kernel, nz, ny),
        out_shape=(vmem(ranks.shape, i32), vmem((1, 128), f32)),
        in_specs=[pl.BlockSpec(memory_space=pl.ANY)] * 3,
        out_specs=(pl.BlockSpec(memory_space=pltpu.VMEM), pl.BlockSpec(memory_space=pltpu.VMEM)),
        scratch_shapes=scratch,
        compiler_params=pltpu.CompilerParams(collective_id=0, has_side_effects=True),
    )(ranks, seeds, flags)
    return pl.pallas_call(
        deliver,
        out_shape=(jax.ShapeDtypeStruct(ranks.shape, i32), jax.ShapeDtypeStruct((ROUNDS,), i32)),
        in_specs=[pl.BlockSpec(memory_space=pltpu.VMEM)] * 2,
        out_specs=(pl.BlockSpec(memory_space=pl.ANY), pl.BlockSpec(memory_space=pltpu.SMEM)),
        scratch_shapes=[dma],
    )(*[pltpu.with_memory_space_constraint(x, pltpu.VMEM) for x in (state, totals)])


def solution(mesh):
    nz, ny = mesh.shape["gz"], mesh.shape["gy"]
    return jax.shard_map(
        functools.partial(per_device, nz, ny), mesh=mesh,
        in_specs=(P("gz", "gy", None), P(None, "gz", "gy", None), P("gz", "gy", None)),
        out_specs=(P("gz", "gy", None), P()), check_vma=False,
    )
```

```python
import functools

import jax
import jax.numpy as jnp
from jax import lax
from jax.experimental import pallas as pl
from jax.experimental.pallas import tpu as pltpu
from jax.sharding import PartitionSpec as P

ROUNDS = 3
EARLY = 1
MESH = pl.DeviceIdType.MESH
UP_UP, UP_DOWN, DOWN_UP, DOWN_DOWN = (1, 1), (1, -1), (-1, 1), (-1, -1)
DIAGONALS = (UP_UP, UP_DOWN, DOWN_UP, DOWN_DOWN)
DIRECTIONS = ((1, 0), (-1, 0), (0, 1), (0, -1)) + DIAGONALS
NONE = -3.0
LINK_Y, DEP_Y = 1 << 12, 1 << 13


def kernel(
    nz, ny,
    ranks_hbm, seeds_hbm, flags_hbm,
    state_ref, totals_ref,
    ranks, seeds, flags,
    bits, partial, rowmax, below, edge_y_out, edge_y_in, edge_d_out, edge_d_in,
    packed, near, near_halo, newc, row_out, row_in, diag_out, diag_in,
    couple, single, whole,
    known, load_sem, edge_send, edge_recv, round_send, round_recv, pair_send, pair_recv, one_send, one_recv, all_send, all_recv,
):
    gz, gy = lax.axis_index("gz"), lax.axis_index("gy")
    depth, rows, width = ranks.shape
    top, end = depth - 1, rows - 1

    loads = [
        pltpu.make_async_copy(seeds_hbm, seeds, load_sem.at[0]),
        pltpu.make_async_copy(ranks_hbm, ranks, load_sem.at[1]),
        pltpu.make_async_copy(flags_hbm, flags, load_sem.at[2]),
    ]
    for load in loads:
        load.start()

    def exists(dz, dy):
        here = None
        for at, step, count in ((gz, dz, nz), (gy, dy, ny)):
            if step:
                inside = at < count - 1 if step > 0 else at > 0
                here = inside if here is None else here & inside
        return here

    there = {d: exists(*d) for d in DIRECTIONS}
    target = {d: (gz + d[0], gy + d[1]) for d in DIRECTIONS}

    barrier = pltpu.get_barrier_semaphore()
    for d in DIAGONALS:
        @pl.when(there[d])
        def _(d=d):
            pl.semaphore_signal(barrier, inc=1, device_id=target[d], device_id_type=MESH)

    for step in (1, nz - 1):
        pl.semaphore_signal(barrier, inc=1, device_id=(lax.rem(gz + step, nz), gy), device_id_type=MESH)

    @pl.loop(1, ny)
    def _(k):
        pl.semaphore_signal(barrier, inc=1, device_id=(gz, lax.rem(gy + k, ny)), device_id_type=MESH)

    strides, reach = [], 1
    while 2 * reach - 1 < nz:
        strides.append(reach)
        reach *= 2

    def tell(i):
        if i < len(strides):
            for step in (strides[i], nz - strides[i]):
                pl.semaphore_signal(known.at[i], inc=1, device_id=(lax.rem(gz + step, nz), gy), device_id_type=MESH)

    def told(i):
        if i < len(strides):
            pl.semaphore_wait(known.at[i], 2)

    def one(flag):
        return jnp.where(flag, 1, 0).astype(jnp.int32)

    sides_z = one(there[(1, 0)]) + one(there[(-1, 0)])
    sides_y = one(there[(0, 1)]) + one(there[(0, -1)])

    started = []

    def remote(direction, source, target_ref, send, recv):
        copy = pltpu.make_async_remote_copy(
            src_ref=source, dst_ref=target_ref, send_sem=send, recv_sem=recv,
            device_id=target[direction], device_id_type=MESH,
        )

        @pl.when(there[direction])
        def _():
            copy.start()

        started.append((direction, copy))
        return direction, copy

    def arrived(pair):
        (dz, dy), copy = pair

        @pl.when(there[(-dz, -dy)])
        def _():
            copy.wait_recv()

    xpos = lax.broadcasted_iota(jnp.int32, (rows, width), 1)
    ypos = lax.broadcasted_iota(jnp.int32, (rows, width), 0)
    first, last = ypos == 0, ypos == end

    def over(row, where, plane):
        return jnp.where(where, jnp.broadcast_to(row, plane.shape), plane)

    def east(plane):
        return pltpu.roll(plane, width - 1, 1)

    def west(plane):
        return pltpu.roll(plane, 1, 1)

    def north(plane):
        return pltpu.roll(plane, rows - 1, 0)

    def south(plane):
        return pltpu.roll(plane, 1, 0)

    zero = jnp.zeros((rows, width), jnp.float32)

    loads[0].wait()

    def in_plane(z):
        c0 = jnp.where(xpos < width - 1, seeds[0, z], 0.0)
        c2 = jnp.where(last & (gy == ny - 1), 0.0, seeds[1, z])
        c4 = seeds[2, z]
        c4 = jnp.where((gz == nz - 1) & (z == top), zero, c4)
        return c0, c2, c4

    def part(z):
        c0, c2, c4 = in_plane(z)
        m = jnp.maximum(jnp.maximum(c0, west(c0)), jnp.maximum(c2, c4))
        m = jnp.maximum(m, jnp.where(first, 0.0, south(c2)))
        if not isinstance(z, int) or z > 0:
            m = jnp.maximum(m, seeds[2, z - 1])
        partial[z + 1] = m
        edge_y_out[0, z] = seeds[1, z, end:rows, :]
        edge_y_out[1, z] = m[end:rows]
        edge_y_out[2, z] = m[0:1]

    part(top)
    part(0)
    edge_d_out[0] = seeds[1, top, end:rows, :]
    edge_d_out[1] = seeds[2, top, end:rows, :]
    edge_d_out[2] = seeds[2, top, 0:1, :]
    edge_d_out[3] = seeds[1, 0, end:rows, :]

    pl.semaphore_wait(barrier, 2 + ny - 1 + sides_z * sides_y)

    def edge(direction, source, target_ref, i):
        return remote(direction, source, target_ref, edge_send.at[i], edge_recv.at[i])

    edge_d = [
        edge(UP_UP, edge_d_out.at[0:2], edge_d_in.at[0:2], 0),
        edge(UP_DOWN, edge_d_out.at[2:3], edge_d_in.at[2:3], 1),
        edge(DOWN_UP, edge_d_out.at[3:4], edge_d_in.at[3:4], 2),
    ]
    edge_z = [
        edge((1, 0), seeds.at[2, top], below, 3),
        edge((1, 0), partial.at[depth], partial.at[0], 4),
        edge((-1, 0), partial.at[1], partial.at[depth + 1], 5),
    ]
    tell(0)
    for z in range(1, top):
        part(z)
    edge_y = [
        edge((0, 1), edge_y_out.at[0:2], edge_y_in.at[0:2], 6),
        edge((0, -1), edge_y_out.at[2:3], edge_y_in.at[2:3], 7),
    ]

    def fill(direction, *refs_values):
        @pl.when(jnp.logical_not(there[direction]))
        def _():
            for ref, value in refs_values:
                ref[...] = jnp.full(ref.shape, value, ref.dtype)

    fill((-1, 0), (below, 0.0), (partial.at[0], 0.0), *[(packed.at[r, 0], NONE) for r in range(ROUNDS)],
         *[(near_halo.at[r, 0], NONE) for r in range(ROUNDS)])
    fill((1, 0), (partial.at[depth + 1], 0.0), *[(packed.at[r, depth + 1], NONE) for r in range(ROUNDS)],
         *[(near_halo.at[r, 1], NONE) for r in range(ROUNDS)])
    fill((0, -1), (edge_y_in.at[0:2], 0.0), *[(row_in.at[r, 0], NONE) for r in range(ROUNDS)])
    fill((0, 1), (edge_y_in.at[2:3], 0.0), *[(row_in.at[r, 1], NONE) for r in range(ROUNDS)])
    fill(DOWN_DOWN, (edge_d_in.at[0:2], 0.0))
    fill(DOWN_UP, (edge_d_in.at[2:3], 0.0))
    fill(UP_DOWN, (edge_d_in.at[3:4], 0.0))
    for i, d in enumerate(DIAGONALS):
        fill((-d[0], -d[1]), *[(diag_in.at[r, i], NONE) for r in range(ROUNDS)])

    def whole_rowmax(z):
        m = jnp.maximum(partial[z + 1], jnp.where(first, jnp.broadcast_to(edge_y_in[0, z], zero.shape), 0.0))
        if z == 0:
            m = jnp.maximum(m, below[...])
        rowmax[z + 1] = m

    def outside_rowmax():
        m = partial[0]
        rowmax[0] = jnp.maximum(m, jnp.where(first, jnp.broadcast_to(edge_d_in[0], zero.shape), 0.0))
        m = jnp.maximum(partial[depth + 1], in_plane(top)[2])
        rowmax[depth + 1] = jnp.maximum(m, jnp.where(first, jnp.broadcast_to(edge_d_in[3], zero.shape), 0.0))

    def strengths(z):
        c0, c2, c4 = in_plane(z)
        c1 = west(c0)
        c3 = over(edge_y_in[0, z], first, south(c2))
        c5 = below[...] if z == 0 else seeds[2, z - 1]
        mine = rowmax[z + 1]
        low = edge_y_in[1, z]
        high = jnp.maximum(edge_y_in[2, z], c2[end:rows])
        if z == 0:
            low = jnp.maximum(low, edge_d_in[1])
            high = jnp.maximum(high, edge_d_in[2])
        others = [
            east(mine), west(mine), over(high, last, north(mine)), over(low, first, south(mine)),
            rowmax[z + 2], rowmax[z],
        ]
        word = jnp.zeros((rows, width), jnp.int32)
        measure = ranks[z]
        outer_link = outer_dep = None
        for d, (cost, other) in enumerate(zip((c0, c1, c2, c3, c4, c5), others)):
            twice = 2.0 * cost
            depends = (cost > 0) & (twice >= mine)
            feeds = (cost > 0) & (twice >= other)
            measure = jnp.where(feeds, 2.0 * measure, measure)
            link = depends | feeds
            if d in (2, 3):
                border = last if d == 2 else first
                outer = jnp.where(link & border, LINK_Y, 0) + jnp.where(depends & border, DEP_Y, 0)
                word = word + outer
                link = link & jnp.logical_not(border)
                depends = depends & jnp.logical_not(border)
            word = word + jnp.where(link, 1 << d, 0) + jnp.where(depends, 1 << (d + 6), 0)
        bits[z] = word
        flag = flags[z]
        packed[0, z + 1] = jnp.where(flag == 0, measure, jnp.where(flag == 2, -2.0, -1.0))

    def linked(word, mask, value):
        return jnp.where((word & mask) != 0, value, NONE)

    def near_inside(r, z):
        word, here = bits[z], packed[r, z + 1]
        m = jnp.maximum(linked(word, 1, east(here)), linked(word, 2, west(here)))
        m = jnp.maximum(m, linked(word, 4, north(here)))
        m = jnp.maximum(m, linked(word, 8, south(here)))
        if z < top:
            m = jnp.maximum(m, linked(word, 16, packed[r, z + 2]))
        if z > 0:
            m = jnp.maximum(m, linked(word, 32, packed[r, z]))
        near[r, z] = m
        for arr, plane in ((0, here), (1, m)):
            row_out[r, 0, arr, z] = plane[end:rows]
            row_out[r, 1, arr, z] = plane[0:1]

    def corner(r, i, d):
        z, row, z_mask = (top if d[0] > 0 else 0), (end if d[1] > 0 else 0), (16 if d[0] > 0 else 32)
        word, value = bits[z, row : row + 1, :], packed[r, z + 1, row : row + 1, :]
        diag_out[r, i, 0] = linked(word, LINK_Y, value)
        diag_out[r, i, 1] = linked(word, z_mask, value)

    def send_packed(r):
        send, recv = round_send.at[r], round_recv.at[r]
        for i, d in enumerate(DIAGONALS):
            corner(r, i, d)
        return [
            *[remote(d, diag_out.at[r, i], diag_in.at[r, i], send.at[6 + i], recv.at[6 + i]) for i, d in enumerate(DIAGONALS)],
            remote((1, 0), packed.at[r, depth], packed.at[r, 0], send.at[0], recv.at[0]),
            remote((-1, 0), packed.at[r, 1], packed.at[r, depth + 1], send.at[2], recv.at[2]),
        ]

    def send_near(r):
        send, recv = round_send.at[r], round_recv.at[r]
        return [
            remote((1, 0), near.at[r, top], near_halo.at[r, 0], send.at[1], recv.at[1]),
            remote((-1, 0), near.at[r, 0], near_halo.at[r, 1], send.at[3], recv.at[3]),
        ]

    def send_rows(r):
        send, recv = round_send.at[r], round_recv.at[r]
        return [
            remote((0, 1), row_out.at[r, 0], row_in.at[r, 0], send.at[4], recv.at[4]),
            remote((0, -1), row_out.at[r, 1], row_in.at[r, 1], send.at[5], recv.at[5]),
        ]

    def yes(mask):
        return jnp.where(mask, -1, 0).astype(jnp.int32)

    def halo_rows(r, arr, z):
        low = jnp.broadcast_to(row_in[r, 0, arr, z], (rows, width))
        return over(row_in[r, 1, arr, z], last, low)

    def finish_near(r, z):
        word, here = bits[z], packed[r, z + 1]
        m = jnp.maximum(near[r, z], linked(word, LINK_Y, halo_rows(r, 0, z)))
        if z == top:
            m = jnp.maximum(m, linked(word, 16, packed[r, z + 2]))
        if z == 0:
            m = jnp.maximum(m, linked(word, 32, packed[r, z]))
        newc[z + 1] = yes((here >= 0) & (here > m))

    def outside_z(r, low):
        z, at, mask = (0, 0, 32) if low else (top, depth + 1, 16)
        there_packed, mine = packed[r, at], packed[r, z + 1]
        limit = jnp.maximum(near_halo[r, 0 if low else 1], linked(bits[z], mask, mine))
        i, j = (0, 1) if low else (2, 3)
        limit = jnp.where(first, jnp.maximum(limit, jnp.broadcast_to(diag_in[r, i, 0], limit.shape)), limit)
        limit = jnp.where(last, jnp.maximum(limit, jnp.broadcast_to(diag_in[r, j, 0], limit.shape)), limit)
        newc[at] = yes((there_packed >= 0) & (there_packed > limit))

    def update(r, z, count):
        word, here, chosen = bits[z], packed[r, z + 1], newc[z + 1]
        outer, limit = halo_rows(r, 0, z), halo_rows(r, 1, z)
        limit = jnp.maximum(limit, linked(word, LINK_Y, here))
        if z in (0, top):
            i, j = (0, 1) if z == 0 else (2, 3)
            corner_value = over(diag_in[r, j, 1], last, jnp.broadcast_to(diag_in[r, i, 1], (rows, width)))
            limit = jnp.maximum(limit, corner_value)
        hit = word & DEP_Y & yes((outer >= 0) & (outer > limit))
        for d, value in enumerate((east(chosen), west(chosen), north(chosen), south(chosen), newc[z + 2], newc[z])):
            hit = hit | (word & (1 << (d + 6)) & value)
        after = jnp.where(chosen != 0, -2.0, jnp.where((here >= 0) & (hit != 0), -1.0, here))
        if r + 1 < ROUNDS:
            packed[r + 1, z + 1] = after
        else:
            state_ref[z] = jnp.where(after >= 0, 0, jnp.where(after == -2.0, 2, 1)).astype(jnp.int32)
        return count + jnp.where(after >= 0, 1.0, 0.0)

    def wait_all(pairs):
        for pair in pairs:
            arrived(pair)

    inner, middle = range(1, top), range(2, top - 1)
    loads[1].wait()
    loads[2].wait()
    wait_all(edge_y)
    for z in inner:
        whole_rowmax(z)
    for z in middle:
        strengths(z)
    wait_all(edge_z)
    wait_all(edge_d)
    whole_rowmax(0)
    whole_rowmax(top)
    outside_rowmax()
    strengths(0)
    strengths(top)

    lane = lax.broadcasted_iota(jnp.int32, (1, 128), 1)
    counted = jnp.zeros((1, 128), jnp.float32)

    def with_count(r):
        total = jnp.sum(jnp.sum(count, axis=0, keepdims=True), axis=1, keepdims=True)
        return jnp.where(lane == r, jnp.broadcast_to(total, counted.shape), counted)

    for r in range(ROUNDS):
        sent_packed = send_packed(r)
        if r == 0:
            strengths(1)
            strengths(top - 1)
        near_inside(r, 0)
        near_inside(r, top)
        sent_near = send_near(r)
        for z in inner:
            near_inside(r, z)
        sent_rows = send_rows(r)
        if r:
            counted = with_count(r - 1)
        told(r)
        tell(r + 1)

        wait_all(sent_rows)
        if r == ROUNDS - 1:
            told(r + 1)
            tell(r + 2)
        for z in inner:
            finish_near(r, z)
        count = zero
        for z in middle:
            count = update(r, z, count)
        wait_all(sent_packed)
        finish_near(r, 0)
        finish_near(r, top)
        count = update(r, 1, count)
        count = update(r, top - 1, count)
        wait_all(sent_near)
        outside_z(r, True)
        outside_z(r, False)
        count = update(r, 0, count)
        count = update(r, top, count)

    half, devices = ny // 2, nz * ny
    column = 8 if nz % 8 == 0 else nz
    columns, early = nz // column, EARLY if column > EARLY else 1
    chip, core, me = gz * half + gy // 2, lax.rem(gy, 2), gz * ny + gy
    is_early = lax.rem(gz, column) < early
    n_early = columns * early * ny
    counted = with_count(ROUNDS - 1)
    couple[core] = counted
    to_partner = pltpu.make_async_remote_copy(
        src_ref=couple.at[core], dst_ref=couple.at[core], send_sem=pair_send, recv_sem=pair_recv,
        device_id=(gz, gy + 1 - 2 * core), device_id_type=MESH)
    to_partner.start()
    told(ROUNDS + 1)

    def at_place(i):
        return lax.rem(i, columns) * column + i // columns

    @pl.loop(0, columns * early)
    def _(i):
        to_z = at_place(i)
        for to_y in range(ny):
            @pl.when((to_z != gz) | (to_y != gy))
            def _():
                pltpu.make_async_remote_copy(
                    src_ref=couple.at[core], dst_ref=single.at[me], send_sem=one_send, recv_sem=one_recv,
                    device_id=(to_z, to_y), device_id_type=MESH).start()

    to_partner.wait_recv()
    whole[chip] = couple[0] + couple[1]

    @pl.loop(columns * early, nz)
    def _(i):
        to_z = at_place(i)
        for pair in range(half):
            @pl.when((to_z != gz) | (pair != gy // 2))
            def _():
                pltpu.make_async_remote_copy(
                    src_ref=whole.at[chip], dst_ref=whole.at[chip], send_sem=all_send, recv_sem=all_recv,
                    device_id=(to_z, 2 * pair + core), device_id_type=MESH).start()

    def passed(buffer, count, sem):
        part = buffer.at[0:count]
        pltpu.make_async_copy(part, part, sem).wait()

    for (dz, dy), copy in started:
        @pl.when(there[(dz, dy)])
        def _(copy=copy):
            copy.wait_send()
    to_partner.wait_send()

    @pl.when(is_early)
    def _():
        single[me] = counted
        passed(single, n_early - 1, one_send)
        passed(whole, (devices - n_early) // 2, all_send)
        passed(single, devices - 1, one_recv)
        totals_ref[...] = jnp.sum(single[...], axis=0)

    @pl.when(jnp.logical_not(is_early))
    def _():
        passed(single, n_early, one_send)
        passed(whole, (devices - n_early) // 2 - 1, all_send)
        passed(whole, devices // 2 - 1, all_recv)
        totals_ref[...] = jnp.sum(whole[...], axis=0)


def deliver(state, totals, state_out, totals_out, numbers, sems):
    whole_state = pltpu.make_async_copy(state, state_out, sems.at[0])
    whole_state.start()
    row = totals[...]
    lane = lax.broadcasted_iota(jnp.int32, row.shape, 1)
    for r in range(ROUNDS):
        numbers[r] = jnp.sum(jnp.where(lane == r, row, 0.0)).astype(jnp.int32)
    all_numbers = pltpu.make_async_copy(numbers, totals_out, sems.at[1])
    all_numbers.start()
    whole_state.wait()
    all_numbers.wait()


def per_device(nz, ny, ranks, seeds, flags):
    depth, rows, width = ranks.shape
    f32, i32, vmem, dma = jnp.float32, jnp.int32, pltpu.VMEM, pltpu.SemaphoreType.DMA
    plane = (rows, width)
    scratch = [
        vmem(ranks.shape, f32), vmem(seeds.shape, f32), vmem(flags.shape, i32),
        vmem(ranks.shape, i32), vmem((depth + 2, *plane), f32), vmem((depth + 2, *plane), f32), vmem(plane, f32),
        vmem((3, depth, 1, width), f32), vmem((3, depth, 1, width), f32),
        vmem((4, 1, width), f32), vmem((4, 1, width), f32),
        vmem((ROUNDS, depth + 2, *plane), f32), vmem((ROUNDS, depth, *plane), f32), vmem((ROUNDS, 2, *plane), f32),
        vmem((depth + 2, *plane), i32),
        vmem((ROUNDS, 2, 2, depth, 1, width), f32), vmem((ROUNDS, 2, 2, depth, 1, width), f32),
        vmem((ROUNDS, 4, 2, 1, width), f32), vmem((ROUNDS, 4, 2, 1, width), f32),
        vmem((2, 1, 128), f32), vmem((nz * ny, 1, 128), f32), vmem((nz * ny // 2, 1, 128), f32),
        pltpu.SemaphoreType.REGULAR((ROUNDS + 2,)), dma((3,)), dma((8,)), dma((8,)), dma((ROUNDS, 10)), dma((ROUNDS, 10)),
        dma, dma, dma, dma, dma, dma,
    ]
    state, totals = pl.pallas_call(
        functools.partial(kernel, nz, ny),
        out_shape=(vmem(ranks.shape, i32), vmem((1, 128), f32)),
        in_specs=[pl.BlockSpec(memory_space=pl.ANY)] * 3,
        out_specs=(pl.BlockSpec(memory_space=pltpu.VMEM), pl.BlockSpec(memory_space=pltpu.VMEM)),
        scratch_shapes=scratch,
        compiler_params=pltpu.CompilerParams(collective_id=0, has_side_effects=True),
    )(ranks, seeds, flags)
    return pl.pallas_call(
        deliver,
        out_shape=(jax.ShapeDtypeStruct(ranks.shape, i32), jax.ShapeDtypeStruct((ROUNDS,), i32)),
        in_specs=[pl.BlockSpec(memory_space=pltpu.VMEM)] * 2,
        out_specs=(pl.BlockSpec(memory_space=pl.ANY), pl.BlockSpec(memory_space=pl.ANY)),
        scratch_shapes=[pltpu.SMEM((ROUNDS,), i32), dma((2,))],
    )(*[pltpu.with_memory_space_constraint(x, pltpu.VMEM) for x in (state, totals)])


def solution(mesh):
    nz, ny = mesh.shape["gz"], mesh.shape["gy"]
    return jax.shard_map(
        functools.partial(per_device, nz, ny), mesh=mesh,
        in_specs=(P("gz", "gy", None), P(None, "gz", "gy", None), P("gz", "gy", None)),
        out_specs=(P("gz", "gy", None), P()), check_vma=False,
    )
```

```python
import functools

import jax
import jax.numpy as jnp
from jax import lax
from jax.experimental import pallas as pl
from jax.experimental.pallas import tpu as pltpu
from jax.sharding import PartitionSpec as P

ROUNDS = 3
EARLY = 1
MESH = pl.DeviceIdType.MESH
UP_UP, UP_DOWN, DOWN_UP, DOWN_DOWN = (1, 1), (1, -1), (-1, 1), (-1, -1)
DIAGONALS = (UP_UP, UP_DOWN, DOWN_UP, DOWN_DOWN)
DIRECTIONS = ((1, 0), (-1, 0), (0, 1), (0, -1)) + DIAGONALS
NONE = -3.0
LINK_Y, DEP_Y = 1 << 12, 1 << 13


def kernel(
    nz, ny,
    ranks_hbm, seeds_hbm, flags_hbm,
    state_ref, totals_ref,
    ranks, seeds, flags,
    bits, partial, rowmax, below, edge_y_out, edge_y_in, edge_d_out, edge_d_in,
    packed, near, near_halo, newc, row_out, row_in, diag_out, diag_in,
    couple, single, whole,
    known, load_sem, edge_send, edge_recv, round_send, round_recv, pair_send, pair_recv, one_send, one_recv, all_send, all_recv,
):
    gz, gy = lax.axis_index("gz"), lax.axis_index("gy")
    depth, rows, width = ranks.shape
    top, end = depth - 1, rows - 1

    loads = [
        pltpu.make_async_copy(seeds_hbm, seeds, load_sem.at[0]),
        pltpu.make_async_copy(ranks_hbm, ranks, load_sem.at[1]),
        pltpu.make_async_copy(flags_hbm, flags, load_sem.at[2]),
    ]
    for load in loads:
        load.start()

    def exists(dz, dy):
        here = None
        for at, step, count in ((gz, dz, nz), (gy, dy, ny)):
            if step:
                inside = at < count - 1 if step > 0 else at > 0
                here = inside if here is None else here & inside
        return here

    there = {d: exists(*d) for d in DIRECTIONS}
    target = {d: (gz + d[0], gy + d[1]) for d in DIRECTIONS}

    barrier = pltpu.get_barrier_semaphore()
    for d in DIAGONALS:
        @pl.when(there[d])
        def _(d=d):
            pl.semaphore_signal(barrier, inc=1, device_id=target[d], device_id_type=MESH)

    for step in (1, nz - 1):
        pl.semaphore_signal(barrier, inc=1, device_id=(lax.rem(gz + step, nz), gy), device_id_type=MESH)

    @pl.loop(1, ny)
    def _(k):
        pl.semaphore_signal(barrier, inc=1, device_id=(gz, lax.rem(gy + k, ny)), device_id_type=MESH)

    strides, reach = [], 1
    while 2 * reach - 1 < nz:
        strides.append(reach)
        reach *= 2

    def tell(i):
        if i < len(strides):
            for step in (strides[i], nz - strides[i]):
                pl.semaphore_signal(known.at[i], inc=1, device_id=(lax.rem(gz + step, nz), gy), device_id_type=MESH)

    def told(i):
        if i < len(strides):
            pl.semaphore_wait(known.at[i], 2)

    def one(flag):
        return jnp.where(flag, 1, 0).astype(jnp.int32)

    sides_z = one(there[(1, 0)]) + one(there[(-1, 0)])
    sides_y = one(there[(0, 1)]) + one(there[(0, -1)])

    started = []

    def remote(direction, source, target_ref, send, recv):
        copy = pltpu.make_async_remote_copy(
            src_ref=source, dst_ref=target_ref, send_sem=send, recv_sem=recv,
            device_id=target[direction], device_id_type=MESH,
        )

        @pl.when(there[direction])
        def _():
            copy.start()

        started.append((direction, copy))
        return direction, copy

    def arrived(pair):
        (dz, dy), copy = pair

        @pl.when(there[(-dz, -dy)])
        def _():
            copy.wait_recv()

    xpos = lax.broadcasted_iota(jnp.int32, (rows, width), 1)
    ypos = lax.broadcasted_iota(jnp.int32, (rows, width), 0)
    first, last = ypos == 0, ypos == end

    def over(row, where, plane):
        return jnp.where(where, jnp.broadcast_to(row, plane.shape), plane)

    def east(plane):
        return pltpu.roll(plane, width - 1, 1)

    def west(plane):
        return pltpu.roll(plane, 1, 1)

    def north(plane):
        return pltpu.roll(plane, rows - 1, 0)

    def south(plane):
        return pltpu.roll(plane, 1, 0)

    zero = jnp.zeros((rows, width), jnp.float32)

    loads[0].wait()

    def in_plane(z):
        c0 = jnp.where(xpos < width - 1, seeds[0, z], 0.0)
        c2 = jnp.where(last & (gy == ny - 1), 0.0, seeds[1, z])
        c4 = seeds[2, z]
        c4 = jnp.where((gz == nz - 1) & (z == top), zero, c4)
        return c0, c2, c4

    def part(z):
        c0, c2, c4 = in_plane(z)
        m = jnp.maximum(jnp.maximum(c0, west(c0)), jnp.maximum(c2, c4))
        m = jnp.maximum(m, jnp.where(first, 0.0, south(c2)))
        if not isinstance(z, int) or z > 0:
            m = jnp.maximum(m, seeds[2, z - 1])
        partial[z + 1] = m
        edge_y_out[0, z] = seeds[1, z, end:rows, :]
        edge_y_out[1, z] = m[end:rows]
        edge_y_out[2, z] = m[0:1]

    part(top)
    part(0)
    edge_d_out[0] = seeds[1, top, end:rows, :]
    edge_d_out[1] = seeds[2, top, end:rows, :]
    edge_d_out[2] = seeds[2, top, 0:1, :]
    edge_d_out[3] = seeds[1, 0, end:rows, :]

    pl.semaphore_wait(barrier, 2 + ny - 1 + sides_z * sides_y)

    def edge(direction, source, target_ref, i):
        return remote(direction, source, target_ref, edge_send.at[i], edge_recv.at[i])

    edge_d = [
        edge(UP_UP, edge_d_out.at[0:2], edge_d_in.at[0:2], 0),
        edge(UP_DOWN, edge_d_out.at[2:3], edge_d_in.at[2:3], 1),
        edge(DOWN_UP, edge_d_out.at[3:4], edge_d_in.at[3:4], 2),
    ]
    edge_z = [
        edge((1, 0), seeds.at[2, top], below, 3),
        edge((1, 0), partial.at[depth], partial.at[0], 4),
        edge((-1, 0), partial.at[1], partial.at[depth + 1], 5),
    ]
    tell(0)
    for z in range(1, top):
        part(z)
    edge_y = [
        edge((0, 1), edge_y_out.at[0:2], edge_y_in.at[0:2], 6),
        edge((0, -1), edge_y_out.at[2:3], edge_y_in.at[2:3], 7),
    ]

    def fill(direction, *refs_values):
        @pl.when(jnp.logical_not(there[direction]))
        def _():
            for ref, value in refs_values:
                ref[...] = jnp.full(ref.shape, value, ref.dtype)

    fill((-1, 0), (below, 0.0), (partial.at[0], 0.0), *[(packed.at[r, 0], NONE) for r in range(ROUNDS)],
         *[(near_halo.at[r, 0], NONE) for r in range(ROUNDS)])
    fill((1, 0), (partial.at[depth + 1], 0.0), *[(packed.at[r, depth + 1], NONE) for r in range(ROUNDS)],
         *[(near_halo.at[r, 1], NONE) for r in range(ROUNDS)])
    fill((0, -1), (edge_y_in.at[0:2], 0.0), *[(row_in.at[r, 0], NONE) for r in range(ROUNDS)])
    fill((0, 1), (edge_y_in.at[2:3], 0.0), *[(row_in.at[r, 1], NONE) for r in range(ROUNDS)])
    fill(DOWN_DOWN, (edge_d_in.at[0:2], 0.0))
    fill(DOWN_UP, (edge_d_in.at[2:3], 0.0))
    fill(UP_DOWN, (edge_d_in.at[3:4], 0.0))
    for i, d in enumerate(DIAGONALS):
        fill((-d[0], -d[1]), *[(diag_in.at[r, i], NONE) for r in range(ROUNDS)])

    def whole_rowmax(z):
        m = jnp.maximum(partial[z + 1], jnp.where(first, jnp.broadcast_to(edge_y_in[0, z], zero.shape), 0.0))
        if z == 0:
            m = jnp.maximum(m, below[...])
        rowmax[z + 1] = m

    def outside_rowmax():
        m = partial[0]
        rowmax[0] = jnp.maximum(m, jnp.where(first, jnp.broadcast_to(edge_d_in[0], zero.shape), 0.0))
        m = jnp.maximum(partial[depth + 1], in_plane(top)[2])
        rowmax[depth + 1] = jnp.maximum(m, jnp.where(first, jnp.broadcast_to(edge_d_in[3], zero.shape), 0.0))

    def strengths(z):
        c0, c2, c4 = in_plane(z)
        c1 = west(c0)
        c3 = over(edge_y_in[0, z], first, south(c2))
        c5 = below[...] if z == 0 else seeds[2, z - 1]
        mine = rowmax[z + 1]
        low = edge_y_in[1, z]
        high = jnp.maximum(edge_y_in[2, z], c2[end:rows])
        if z == 0:
            low = jnp.maximum(low, edge_d_in[1])
            high = jnp.maximum(high, edge_d_in[2])
        others = [
            east(mine), west(mine), over(high, last, north(mine)), over(low, first, south(mine)),
            rowmax[z + 2], rowmax[z],
        ]
        word = jnp.zeros((rows, width), jnp.int32)
        measure = ranks[z]
        outer_link = outer_dep = None
        for d, (cost, other) in enumerate(zip((c0, c1, c2, c3, c4, c5), others)):
            twice = 2.0 * cost
            depends = (cost > 0) & (twice >= mine)
            feeds = (cost > 0) & (twice >= other)
            measure = jnp.where(feeds, 2.0 * measure, measure)
            link = depends | feeds
            if d in (2, 3):
                border = last if d == 2 else first
                outer = jnp.where(link & border, LINK_Y, 0) + jnp.where(depends & border, DEP_Y, 0)
                word = word + outer
                link = link & jnp.logical_not(border)
                depends = depends & jnp.logical_not(border)
            word = word + jnp.where(link, 1 << d, 0) + jnp.where(depends, 1 << (d + 6), 0)
        bits[z] = word
        flag = flags[z]
        packed[0, z + 1] = jnp.where(flag == 0, measure, jnp.where(flag == 2, -2.0, -1.0))

    def linked(word, mask, value):
        return jnp.where((word & mask) != 0, value, NONE)

    def near_inside(r, z):
        word, here = bits[z], packed[r, z + 1]
        m = jnp.maximum(linked(word, 1, east(here)), linked(word, 2, west(here)))
        m = jnp.maximum(m, linked(word, 4, north(here)))
        m = jnp.maximum(m, linked(word, 8, south(here)))
        if z < top:
            m = jnp.maximum(m, linked(word, 16, packed[r, z + 2]))
        if z > 0:
            m = jnp.maximum(m, linked(word, 32, packed[r, z]))
        near[r, z] = m
        for arr, plane in ((0, here), (1, m)):
            row_out[r, 0, arr, z] = plane[end:rows]
            row_out[r, 1, arr, z] = plane[0:1]

    def corner(r, i, d):
        z, row, z_mask = (top if d[0] > 0 else 0), (end if d[1] > 0 else 0), (16 if d[0] > 0 else 32)
        word, value = bits[z, row : row + 1, :], packed[r, z + 1, row : row + 1, :]
        diag_out[r, i, 0] = linked(word, LINK_Y, value)
        diag_out[r, i, 1] = linked(word, z_mask, value)

    def send_packed(r, low):
        send, recv = round_send.at[r], round_recv.at[r]
        if low:
            return remote((-1, 0), packed.at[r, 1], packed.at[r, depth + 1], send.at[2], recv.at[2])
        return remote((1, 0), packed.at[r, depth], packed.at[r, 0], send.at[0], recv.at[0])

    def send_diag(r):
        send, recv = round_send.at[r], round_recv.at[r]
        for i, d in enumerate(DIAGONALS):
            corner(r, i, d)
        return [remote(d, diag_out.at[r, i], diag_in.at[r, i], send.at[6 + i], recv.at[6 + i]) for i, d in enumerate(DIAGONALS)]

    def send_near(r, low):
        send, recv = round_send.at[r], round_recv.at[r]
        if low:
            return remote((-1, 0), near.at[r, 0], near_halo.at[r, 1], send.at[3], recv.at[3])
        return remote((1, 0), near.at[r, top], near_halo.at[r, 0], send.at[1], recv.at[1])

    def send_rows(r):
        send, recv = round_send.at[r], round_recv.at[r]
        return [
            remote((0, 1), row_out.at[r, 0], row_in.at[r, 0], send.at[4], recv.at[4]),
            remote((0, -1), row_out.at[r, 1], row_in.at[r, 1], send.at[5], recv.at[5]),
        ]

    def yes(mask):
        return jnp.where(mask, -1, 0).astype(jnp.int32)

    def halo_rows(r, arr, z):
        low = jnp.broadcast_to(row_in[r, 0, arr, z], (rows, width))
        return over(row_in[r, 1, arr, z], last, low)

    def finish_near(r, z):
        word, here = bits[z], packed[r, z + 1]
        m = jnp.maximum(near[r, z], linked(word, LINK_Y, halo_rows(r, 0, z)))
        if z == top:
            m = jnp.maximum(m, linked(word, 16, packed[r, z + 2]))
        if z == 0:
            m = jnp.maximum(m, linked(word, 32, packed[r, z]))
        newc[z + 1] = yes((here >= 0) & (here > m))

    def outside_z(r, low):
        z, at, mask = (0, 0, 32) if low else (top, depth + 1, 16)
        there_packed, mine = packed[r, at], packed[r, z + 1]
        limit = jnp.maximum(near_halo[r, 0 if low else 1], linked(bits[z], mask, mine))
        i, j = (0, 1) if low else (2, 3)
        limit = jnp.where(first, jnp.maximum(limit, jnp.broadcast_to(diag_in[r, i, 0], limit.shape)), limit)
        limit = jnp.where(last, jnp.maximum(limit, jnp.broadcast_to(diag_in[r, j, 0], limit.shape)), limit)
        newc[at] = yes((there_packed >= 0) & (there_packed > limit))

    def update(r, z, count):
        word, here, chosen = bits[z], packed[r, z + 1], newc[z + 1]
        outer, limit = halo_rows(r, 0, z), halo_rows(r, 1, z)
        limit = jnp.maximum(limit, linked(word, LINK_Y, here))
        if z in (0, top):
            i, j = (0, 1) if z == 0 else (2, 3)
            corner_value = over(diag_in[r, j, 1], last, jnp.broadcast_to(diag_in[r, i, 1], (rows, width)))
            limit = jnp.maximum(limit, corner_value)
        hit = word & DEP_Y & yes((outer >= 0) & (outer > limit))
        for d, value in enumerate((east(chosen), west(chosen), north(chosen), south(chosen), newc[z + 2], newc[z])):
            hit = hit | (word & (1 << (d + 6)) & value)
        after = jnp.where(chosen != 0, -2.0, jnp.where((here >= 0) & (hit != 0), -1.0, here))
        if r + 1 < ROUNDS:
            packed[r + 1, z + 1] = after
        else:
            state_ref[z] = jnp.where(after >= 0, 0, jnp.where(after == -2.0, 2, 1)).astype(jnp.int32)
        return count + jnp.where(after >= 0, 1.0, 0.0)

    def wait_all(pairs):
        for pair in pairs:
            arrived(pair)

    inner, middle = range(1, top), range(2, top - 1)
    loads[1].wait()
    loads[2].wait()
    wait_all(edge_y)
    for z in inner:
        whole_rowmax(z)
    for z in middle:
        strengths(z)
    wait_all(edge_z)
    wait_all(edge_d)
    whole_rowmax(0)
    whole_rowmax(top)
    outside_rowmax()
    strengths(0)
    strengths(top)

    lane = lax.broadcasted_iota(jnp.int32, (1, 128), 1)
    counted = jnp.zeros((1, 128), jnp.float32)

    def with_count(r):
        total = jnp.sum(jnp.sum(count, axis=0, keepdims=True), axis=1, keepdims=True)
        return jnp.where(lane == r, jnp.broadcast_to(total, counted.shape), counted)

    packed_down, packed_up = send_packed(0, True), send_packed(0, False)
    for r in range(ROUNDS):
        sent_diag = send_diag(r)
        if r == 0:
            strengths(1)
            strengths(top - 1)
        near_inside(r, 0)
        near_down = send_near(r, True)
        near_inside(r, top)
        near_up = send_near(r, False)
        for z in inner:
            near_inside(r, z)
        sent_rows = send_rows(r)
        if r:
            counted = with_count(r - 1)
        told(r)
        tell(r + 1)

        wait_all(sent_rows)
        if r == ROUNDS - 1:
            told(r + 1)
            tell(r + 2)
        for z in inner:
            finish_near(r, z)
        count = zero
        for z in middle:
            count = update(r, z, count)
        arrived(packed_up)
        finish_near(r, 0)
        count = update(r, 1, count)
        arrived(packed_down)
        finish_near(r, top)
        count = update(r, top - 1, count)
        following = []
        for low, z, pair, diagonals in ((True, 0, near_up, sent_diag[:2]), (False, top, near_down, sent_diag[2:])):
            arrived(pair)
            wait_all(diagonals)
            outside_z(r, low)
            count = update(r, z, count)
            if r + 1 < ROUNDS:
                following.append(send_packed(r + 1, low))
        if following:
            packed_down, packed_up = following

    half, devices = ny // 2, nz * ny
    column = 8 if nz % 8 == 0 else nz
    columns, early = nz // column, EARLY if column > EARLY else 1
    chip, core, me = gz * half + gy // 2, lax.rem(gy, 2), gz * ny + gy
    is_early = lax.rem(gz, column) < early
    n_early = columns * early * ny
    counted = with_count(ROUNDS - 1)
    couple[core] = counted
    to_partner = pltpu.make_async_remote_copy(
        src_ref=couple.at[core], dst_ref=couple.at[core], send_sem=pair_send, recv_sem=pair_recv,
        device_id=(gz, gy + 1 - 2 * core), device_id_type=MESH)
    to_partner.start()
    told(ROUNDS + 1)

    def at_place(i):
        return lax.rem(i, columns) * column + i // columns

    @pl.loop(0, columns * early)
    def _(i):
        to_z = at_place(i)
        for to_y in range(ny):
            @pl.when((to_z != gz) | (to_y != gy))
            def _():
                pltpu.make_async_remote_copy(
                    src_ref=couple.at[core], dst_ref=single.at[me], send_sem=one_send, recv_sem=one_recv,
                    device_id=(to_z, to_y), device_id_type=MESH).start()

    to_partner.wait_recv()
    whole[chip] = couple[0] + couple[1]

    @pl.loop(columns * early, nz)
    def _(i):
        to_z = at_place(i)
        for pair in range(half):
            @pl.when((to_z != gz) | (pair != gy // 2))
            def _():
                pltpu.make_async_remote_copy(
                    src_ref=whole.at[chip], dst_ref=whole.at[chip], send_sem=all_send, recv_sem=all_recv,
                    device_id=(to_z, 2 * pair + core), device_id_type=MESH).start()

    def passed(buffer, count, sem):
        part = buffer.at[0:count]
        pltpu.make_async_copy(part, part, sem).wait()

    for (dz, dy), copy in started:
        @pl.when(there[(dz, dy)])
        def _(copy=copy):
            copy.wait_send()
    to_partner.wait_send()

    @pl.when(is_early)
    def _():
        single[me] = counted
        passed(single, n_early - 1, one_send)
        passed(whole, (devices - n_early) // 2, all_send)
        passed(single, devices - 1, one_recv)
        totals_ref[...] = jnp.sum(single[...], axis=0)

    @pl.when(jnp.logical_not(is_early))
    def _():
        passed(single, n_early, one_send)
        passed(whole, (devices - n_early) // 2 - 1, all_send)
        passed(whole, devices // 2 - 1, all_recv)
        totals_ref[...] = jnp.sum(whole[...], axis=0)


def deliver(state, totals, state_out, totals_out, numbers, sems):
    whole_state = pltpu.make_async_copy(state, state_out, sems.at[0])
    whole_state.start()
    row = totals[...]
    lane = lax.broadcasted_iota(jnp.int32, row.shape, 1)
    for r in range(ROUNDS):
        numbers[r] = jnp.sum(jnp.where(lane == r, row, 0.0)).astype(jnp.int32)
    all_numbers = pltpu.make_async_copy(numbers, totals_out, sems.at[1])
    all_numbers.start()
    whole_state.wait()
    all_numbers.wait()


def per_device(nz, ny, ranks, seeds, flags):
    depth, rows, width = ranks.shape
    f32, i32, vmem, dma = jnp.float32, jnp.int32, pltpu.VMEM, pltpu.SemaphoreType.DMA
    plane = (rows, width)
    scratch = [
        vmem(ranks.shape, f32), vmem(seeds.shape, f32), vmem(flags.shape, i32),
        vmem(ranks.shape, i32), vmem((depth + 2, *plane), f32), vmem((depth + 2, *plane), f32), vmem(plane, f32),
        vmem((3, depth, 1, width), f32), vmem((3, depth, 1, width), f32),
        vmem((4, 1, width), f32), vmem((4, 1, width), f32),
        vmem((ROUNDS, depth + 2, *plane), f32), vmem((ROUNDS, depth, *plane), f32), vmem((ROUNDS, 2, *plane), f32),
        vmem((depth + 2, *plane), i32),
        vmem((ROUNDS, 2, 2, depth, 1, width), f32), vmem((ROUNDS, 2, 2, depth, 1, width), f32),
        vmem((ROUNDS, 4, 2, 1, width), f32), vmem((ROUNDS, 4, 2, 1, width), f32),
        vmem((2, 1, 128), f32), vmem((nz * ny, 1, 128), f32), vmem((nz * ny // 2, 1, 128), f32),
        pltpu.SemaphoreType.REGULAR((ROUNDS + 2,)), dma((3,)), dma((8,)), dma((8,)), dma((ROUNDS, 10)), dma((ROUNDS, 10)),
        dma, dma, dma, dma, dma, dma,
    ]
    state, totals = pl.pallas_call(
        functools.partial(kernel, nz, ny),
        out_shape=(vmem(ranks.shape, i32), vmem((1, 128), f32)),
        in_specs=[pl.BlockSpec(memory_space=pl.ANY)] * 3,
        out_specs=(pl.BlockSpec(memory_space=pltpu.VMEM), pl.BlockSpec(memory_space=pltpu.VMEM)),
        scratch_shapes=scratch,
        compiler_params=pltpu.CompilerParams(collective_id=0, has_side_effects=True),
    )(ranks, seeds, flags)
    return pl.pallas_call(
        deliver,
        out_shape=(jax.ShapeDtypeStruct(ranks.shape, i32), jax.ShapeDtypeStruct((ROUNDS,), i32)),
        in_specs=[pl.BlockSpec(memory_space=pltpu.VMEM)] * 2,
        out_specs=(pl.BlockSpec(memory_space=pl.ANY), pl.BlockSpec(memory_space=pl.ANY)),
        scratch_shapes=[pltpu.SMEM((ROUNDS,), i32), dma((2,))],
    )(*[pltpu.with_memory_space_constraint(x, pltpu.VMEM) for x in (state, totals)])


def solution(mesh):
    nz, ny = mesh.shape["gz"], mesh.shape["gy"]
    return jax.shard_map(
        functools.partial(per_device, nz, ny), mesh=mesh,
        in_specs=(P("gz", "gy", None), P(None, "gz", "gy", None), P("gz", "gy", None)),
        out_specs=(P("gz", "gy", None), P()), check_vma=False,
    )
```

```python
import functools

import jax
import jax.numpy as jnp
from jax import lax
from jax.experimental import pallas as pl
from jax.experimental.pallas import tpu as pltpu
from jax.sharding import PartitionSpec as P

ROUNDS = 3
EARLY = 1
MESH = pl.DeviceIdType.MESH
UP_UP, UP_DOWN, DOWN_UP, DOWN_DOWN = (1, 1), (1, -1), (-1, 1), (-1, -1)
DIAGONALS = (UP_UP, UP_DOWN, DOWN_UP, DOWN_DOWN)
DIRECTIONS = ((1, 0), (-1, 0), (0, 1), (0, -1)) + DIAGONALS
NONE = -3.0
LINK_Y, DEP_Y = 1 << 12, 1 << 13


def kernel(
    nz, ny,
    ranks_hbm, seeds_hbm, flags_hbm,
    state_ref, totals_ref,
    ranks, seeds, flags,
    bits, partial, rowmax, below, edge_y_out, edge_y_in, edge_d_out, edge_d_in,
    packed, near, near_halo, newc, row_out, row_in, diag_out, diag_in,
    couple, single, whole,
    known, load_sem, edge_send, edge_recv, round_send, round_recv, pair_send, pair_recv, one_send, one_recv, all_send, all_recv,
):
    gz, gy = lax.axis_index("gz"), lax.axis_index("gy")
    depth, rows, width = ranks.shape
    top, end = depth - 1, rows - 1

    loads = [
        pltpu.make_async_copy(seeds_hbm, seeds, load_sem.at[0]),
        pltpu.make_async_copy(ranks_hbm, ranks, load_sem.at[1]),
        pltpu.make_async_copy(flags_hbm, flags, load_sem.at[2]),
    ]
    for load in loads:
        load.start()

    def exists(dz, dy):
        here = None
        for at, step, count in ((gz, dz, nz), (gy, dy, ny)):
            if step:
                inside = at < count - 1 if step > 0 else at > 0
                here = inside if here is None else here & inside
        return here

    there = {d: exists(*d) for d in DIRECTIONS}
    target = {d: (gz + d[0], gy + d[1]) for d in DIRECTIONS}

    barrier = pltpu.get_barrier_semaphore()
    for d in DIAGONALS:
        @pl.when(there[d])
        def _(d=d):
            pl.semaphore_signal(barrier, inc=1, device_id=target[d], device_id_type=MESH)

    for step in (1, nz - 1):
        pl.semaphore_signal(barrier, inc=1, device_id=(lax.rem(gz + step, nz), gy), device_id_type=MESH)

    @pl.loop(1, ny)
    def _(k):
        pl.semaphore_signal(barrier, inc=1, device_id=(gz, lax.rem(gy + k, ny)), device_id_type=MESH)

    strides, reach = [], 1
    while 2 * reach - 1 < nz:
        strides.append(reach)
        reach *= 2

    def tell(i):
        if i < len(strides):
            for step in (strides[i], nz - strides[i]):
                pl.semaphore_signal(known.at[i], inc=1, device_id=(lax.rem(gz + step, nz), gy), device_id_type=MESH)

    def told(i):
        if i < len(strides):
            pl.semaphore_wait(known.at[i], 2)

    def one(flag):
        return jnp.where(flag, 1, 0).astype(jnp.int32)

    sides_z = one(there[(1, 0)]) + one(there[(-1, 0)])
    sides_y = one(there[(0, 1)]) + one(there[(0, -1)])

    started = []

    def remote(direction, source, target_ref, send, recv):
        copy = pltpu.make_async_remote_copy(
            src_ref=source, dst_ref=target_ref, send_sem=send, recv_sem=recv,
            device_id=target[direction], device_id_type=MESH,
        )

        @pl.when(there[direction])
        def _():
            copy.start()

        started.append((direction, copy))
        return direction, copy

    def arrived(pair):
        (dz, dy), copy = pair

        @pl.when(there[(-dz, -dy)])
        def _():
            copy.wait_recv()

    xpos = lax.broadcasted_iota(jnp.int32, (rows, width), 1)
    ypos = lax.broadcasted_iota(jnp.int32, (rows, width), 0)
    first, last = ypos == 0, ypos == end

    def over(row, where, plane):
        return jnp.where(where, jnp.broadcast_to(row, plane.shape), plane)

    def east(plane):
        return pltpu.roll(plane, width - 1, 1)

    def west(plane):
        return pltpu.roll(plane, 1, 1)

    def north(plane):
        return pltpu.roll(plane, rows - 1, 0)

    def south(plane):
        return pltpu.roll(plane, 1, 0)

    zero = jnp.zeros((rows, width), jnp.float32)

    loads[0].wait()

    def in_plane(z):
        c0 = jnp.where(xpos < width - 1, seeds[0, z], 0.0)
        c2 = jnp.where(last & (gy == ny - 1), 0.0, seeds[1, z])
        c4 = seeds[2, z]
        c4 = jnp.where((gz == nz - 1) & (z == top), zero, c4)
        return c0, c2, c4

    def part(z):
        c0, c2, c4 = in_plane(z)
        m = jnp.maximum(jnp.maximum(c0, west(c0)), jnp.maximum(c2, c4))
        m = jnp.maximum(m, jnp.where(first, 0.0, south(c2)))
        if not isinstance(z, int) or z > 0:
            m = jnp.maximum(m, seeds[2, z - 1])
        partial[z + 1] = m
        edge_y_out[0, z] = seeds[1, z, end:rows, :]
        edge_y_out[1, z] = m[end:rows]
        edge_y_out[2, z] = m[0:1]

    part(top)
    part(0)
    edge_d_out[0] = seeds[1, top, end:rows, :]
    edge_d_out[1] = seeds[2, top, end:rows, :]
    edge_d_out[2] = seeds[2, top, 0:1, :]
    edge_d_out[3] = seeds[1, 0, end:rows, :]

    pl.semaphore_wait(barrier, 2 + ny - 1 + sides_z * sides_y)

    def edge(direction, source, target_ref, i):
        return remote(direction, source, target_ref, edge_send.at[i], edge_recv.at[i])

    edge_d = [
        edge(UP_UP, edge_d_out.at[0:2], edge_d_in.at[0:2], 0),
        edge(UP_DOWN, edge_d_out.at[2:3], edge_d_in.at[2:3], 1),
        edge(DOWN_UP, edge_d_out.at[3:4], edge_d_in.at[3:4], 2),
    ]
    edge_z = [
        edge((1, 0), seeds.at[2, top], below, 3),
        edge((1, 0), partial.at[depth], partial.at[0], 4),
        edge((-1, 0), partial.at[1], partial.at[depth + 1], 5),
    ]
    tell(0)
    for z in range(1, top):
        part(z)
    edge_y = [
        edge((0, 1), edge_y_out.at[0:2], edge_y_in.at[0:2], 6),
        edge((0, -1), edge_y_out.at[2:3], edge_y_in.at[2:3], 7),
    ]

    def fill(direction, *refs_values):
        @pl.when(jnp.logical_not(there[direction]))
        def _():
            for ref, value in refs_values:
                ref[...] = jnp.full(ref.shape, value, ref.dtype)

    fill((-1, 0), (below, 0.0), (partial.at[0], 0.0), *[(packed.at[r, 0], NONE) for r in range(ROUNDS)],
         *[(near_halo.at[r, 0], NONE) for r in range(ROUNDS)])
    fill((1, 0), (partial.at[depth + 1], 0.0), *[(packed.at[r, depth + 1], NONE) for r in range(ROUNDS)],
         *[(near_halo.at[r, 1], NONE) for r in range(ROUNDS)])
    fill((0, -1), (edge_y_in.at[0:2], 0.0), *[(row_in.at[r, 0], NONE) for r in range(ROUNDS)])
    fill((0, 1), (edge_y_in.at[2:3], 0.0), *[(row_in.at[r, 1], NONE) for r in range(ROUNDS)])
    fill(DOWN_DOWN, (edge_d_in.at[0:2], 0.0))
    fill(DOWN_UP, (edge_d_in.at[2:3], 0.0))
    fill(UP_DOWN, (edge_d_in.at[3:4], 0.0))
    for i, d in enumerate(DIAGONALS):
        fill((-d[0], -d[1]), *[(diag_in.at[r, i], NONE) for r in range(ROUNDS)])

    def whole_rowmax(z):
        m = jnp.maximum(partial[z + 1], jnp.where(first, jnp.broadcast_to(edge_y_in[0, z], zero.shape), 0.0))
        if z == 0:
            m = jnp.maximum(m, below[...])
        rowmax[z + 1] = m

    def outside_rowmax(low):
        at, i = (0, 0) if low else (depth + 1, 3)
        m = partial[at] if low else jnp.maximum(partial[at], in_plane(top)[2])
        rowmax[at] = jnp.maximum(m, jnp.where(first, jnp.broadcast_to(edge_d_in[i], zero.shape), 0.0))

    def strengths(z):
        c0, c2, c4 = in_plane(z)
        c1 = west(c0)
        c3 = over(edge_y_in[0, z], first, south(c2))
        c5 = below[...] if z == 0 else seeds[2, z - 1]
        mine = rowmax[z + 1]
        low = edge_y_in[1, z]
        high = jnp.maximum(edge_y_in[2, z], c2[end:rows])
        if z == 0:
            low = jnp.maximum(low, edge_d_in[1])
            high = jnp.maximum(high, edge_d_in[2])
        others = [
            east(mine), west(mine), over(high, last, north(mine)), over(low, first, south(mine)),
            rowmax[z + 2], rowmax[z],
        ]
        word = jnp.zeros((rows, width), jnp.int32)
        measure = ranks[z]
        outer_link = outer_dep = None
        for d, (cost, other) in enumerate(zip((c0, c1, c2, c3, c4, c5), others)):
            twice = 2.0 * cost
            depends = (cost > 0) & (twice >= mine)
            feeds = (cost > 0) & (twice >= other)
            measure = jnp.where(feeds, 2.0 * measure, measure)
            link = depends | feeds
            if d in (2, 3):
                border = last if d == 2 else first
                outer = jnp.where(link & border, LINK_Y, 0) + jnp.where(depends & border, DEP_Y, 0)
                word = word + outer
                link = link & jnp.logical_not(border)
                depends = depends & jnp.logical_not(border)
            word = word + jnp.where(link, 1 << d, 0) + jnp.where(depends, 1 << (d + 6), 0)
        bits[z] = word
        flag = flags[z]
        packed[0, z + 1] = jnp.where(flag == 0, measure, jnp.where(flag == 2, -2.0, -1.0))

    def linked(word, mask, value):
        return jnp.where((word & mask) != 0, value, NONE)

    def near_inside(r, z):
        word, here = bits[z], packed[r, z + 1]
        m = jnp.maximum(linked(word, 1, east(here)), linked(word, 2, west(here)))
        m = jnp.maximum(m, linked(word, 4, north(here)))
        m = jnp.maximum(m, linked(word, 8, south(here)))
        if z < top:
            m = jnp.maximum(m, linked(word, 16, packed[r, z + 2]))
        if z > 0:
            m = jnp.maximum(m, linked(word, 32, packed[r, z]))
        near[r, z] = m
        for arr, plane in ((0, here), (1, m)):
            row_out[r, 0, arr, z] = plane[end:rows]
            row_out[r, 1, arr, z] = plane[0:1]

    def corner(r, i, d):
        z, row, z_mask = (top if d[0] > 0 else 0), (end if d[1] > 0 else 0), (16 if d[0] > 0 else 32)
        word, value = bits[z, row : row + 1, :], packed[r, z + 1, row : row + 1, :]
        diag_out[r, i, 0] = linked(word, LINK_Y, value)
        diag_out[r, i, 1] = linked(word, z_mask, value)

    def send_packed(r, low):
        send, recv = round_send.at[r], round_recv.at[r]
        if low:
            return remote((-1, 0), packed.at[r, 1], packed.at[r, depth + 1], send.at[2], recv.at[2])
        return remote((1, 0), packed.at[r, depth], packed.at[r, 0], send.at[0], recv.at[0])

    def send_diag(r):
        send, recv = round_send.at[r], round_recv.at[r]
        for i, d in enumerate(DIAGONALS):
            corner(r, i, d)
        return [remote(d, diag_out.at[r, i], diag_in.at[r, i], send.at[6 + i], recv.at[6 + i]) for i, d in enumerate(DIAGONALS)]

    def send_near(r, low):
        send, recv = round_send.at[r], round_recv.at[r]
        if low:
            return remote((-1, 0), near.at[r, 0], near_halo.at[r, 1], send.at[3], recv.at[3])
        return remote((1, 0), near.at[r, top], near_halo.at[r, 0], send.at[1], recv.at[1])

    def send_rows(r):
        send, recv = round_send.at[r], round_recv.at[r]
        return [
            remote((0, 1), row_out.at[r, 0], row_in.at[r, 0], send.at[4], recv.at[4]),
            remote((0, -1), row_out.at[r, 1], row_in.at[r, 1], send.at[5], recv.at[5]),
        ]

    def yes(mask):
        return jnp.where(mask, -1, 0).astype(jnp.int32)

    def halo_rows(r, arr, z):
        low = jnp.broadcast_to(row_in[r, 0, arr, z], (rows, width))
        return over(row_in[r, 1, arr, z], last, low)

    def finish_near(r, z):
        word, here = bits[z], packed[r, z + 1]
        m = jnp.maximum(near[r, z], linked(word, LINK_Y, halo_rows(r, 0, z)))
        if z == top:
            m = jnp.maximum(m, linked(word, 16, packed[r, z + 2]))
        if z == 0:
            m = jnp.maximum(m, linked(word, 32, packed[r, z]))
        newc[z + 1] = yes((here >= 0) & (here > m))

    def outside_z(r, low):
        z, at, mask = (0, 0, 32) if low else (top, depth + 1, 16)
        there_packed, mine = packed[r, at], packed[r, z + 1]
        limit = jnp.maximum(near_halo[r, 0 if low else 1], linked(bits[z], mask, mine))
        i, j = (0, 1) if low else (2, 3)
        limit = jnp.where(first, jnp.maximum(limit, jnp.broadcast_to(diag_in[r, i, 0], limit.shape)), limit)
        limit = jnp.where(last, jnp.maximum(limit, jnp.broadcast_to(diag_in[r, j, 0], limit.shape)), limit)
        newc[at] = yes((there_packed >= 0) & (there_packed > limit))

    def update(r, z, count):
        word, here, chosen = bits[z], packed[r, z + 1], newc[z + 1]
        outer, limit = halo_rows(r, 0, z), halo_rows(r, 1, z)
        limit = jnp.maximum(limit, linked(word, LINK_Y, here))
        if z in (0, top):
            i, j = (0, 1) if z == 0 else (2, 3)
            corner_value = over(diag_in[r, j, 1], last, jnp.broadcast_to(diag_in[r, i, 1], (rows, width)))
            limit = jnp.maximum(limit, corner_value)
        hit = word & DEP_Y & yes((outer >= 0) & (outer > limit))
        for d, value in enumerate((east(chosen), west(chosen), north(chosen), south(chosen), newc[z + 2], newc[z])):
            hit = hit | (word & (1 << (d + 6)) & value)
        after = jnp.where(chosen != 0, -2.0, jnp.where((here >= 0) & (hit != 0), -1.0, here))
        if r + 1 < ROUNDS:
            packed[r + 1, z + 1] = after
        else:
            state_ref[z] = jnp.where(after >= 0, 0, jnp.where(after == -2.0, 2, 1)).astype(jnp.int32)
        return count + jnp.where(after >= 0, 1.0, 0.0)

    def wait_all(pairs):
        for pair in pairs:
            arrived(pair)

    inner, middle = range(1, top), range(2, top - 1)
    loads[1].wait()
    loads[2].wait()
    wait_all(edge_y)
    for z in inner:
        whole_rowmax(z)
    for z in middle:
        strengths(z)
    whole_rowmax(top)
    wait_all(edge_z[2:])
    wait_all(edge_d[2:])
    outside_rowmax(False)
    strengths(top)
    packed_up = send_packed(0, False)
    wait_all(edge_z[:2])
    wait_all(edge_d[:2])
    whole_rowmax(0)
    outside_rowmax(True)
    strengths(0)
    packed_down = send_packed(0, True)

    lane = lax.broadcasted_iota(jnp.int32, (1, 128), 1)
    counted = jnp.zeros((1, 128), jnp.float32)

    def with_count(r):
        total = jnp.sum(jnp.sum(count, axis=0, keepdims=True), axis=1, keepdims=True)
        return jnp.where(lane == r, jnp.broadcast_to(total, counted.shape), counted)

    for r in range(ROUNDS):
        sent_diag = send_diag(r)
        if r == 0:
            strengths(1)
            strengths(top - 1)
        near_inside(r, 0)
        near_down = send_near(r, True)
        near_inside(r, top)
        near_up = send_near(r, False)
        for z in inner:
            near_inside(r, z)
        sent_rows = send_rows(r)
        if r:
            counted = with_count(r - 1)
        told(r)
        tell(r + 1)

        wait_all(sent_rows)
        if r == ROUNDS - 1:
            told(r + 1)
            tell(r + 2)
        for z in inner:
            finish_near(r, z)
        count = zero
        for z in middle:
            count = update(r, z, count)
        arrived(packed_up)
        finish_near(r, 0)
        count = update(r, 1, count)
        arrived(packed_down)
        finish_near(r, top)
        count = update(r, top - 1, count)
        following = []
        for low, z, pair, diagonals in ((True, 0, near_up, sent_diag[:2]), (False, top, near_down, sent_diag[2:])):
            arrived(pair)
            wait_all(diagonals)
            outside_z(r, low)
            count = update(r, z, count)
            if r + 1 < ROUNDS:
                following.append(send_packed(r + 1, low))
        if following:
            packed_down, packed_up = following

    half, devices = ny // 2, nz * ny
    column = 8 if nz % 8 == 0 else nz
    columns, early = nz // column, EARLY if column > EARLY else 1
    chip, core, me = gz * half + gy // 2, lax.rem(gy, 2), gz * ny + gy
    is_early = lax.rem(gz, column) < early
    n_early = columns * early * ny
    counted = with_count(ROUNDS - 1)
    couple[core] = counted
    to_partner = pltpu.make_async_remote_copy(
        src_ref=couple.at[core], dst_ref=couple.at[core], send_sem=pair_send, recv_sem=pair_recv,
        device_id=(gz, gy + 1 - 2 * core), device_id_type=MESH)
    to_partner.start()
    told(ROUNDS + 1)

    def at_place(i):
        return lax.rem(i, columns) * column + i // columns

    @pl.loop(0, columns * early)
    def _(i):
        to_z = at_place(i)
        for to_y in range(ny):
            @pl.when((to_z != gz) | (to_y != gy))
            def _():
                pltpu.make_async_remote_copy(
                    src_ref=couple.at[core], dst_ref=single.at[me], send_sem=one_send, recv_sem=one_recv,
                    device_id=(to_z, to_y), device_id_type=MESH).start()

    to_partner.wait_recv()
    whole[chip] = couple[0] + couple[1]

    @pl.loop(columns * early, nz)
    def _(i):
        to_z = at_place(i)
        for pair in range(half):
            @pl.when((to_z != gz) | (pair != gy // 2))
            def _():
                pltpu.make_async_remote_copy(
                    src_ref=whole.at[chip], dst_ref=whole.at[chip], send_sem=all_send, recv_sem=all_recv,
                    device_id=(to_z, 2 * pair + core), device_id_type=MESH).start()

    def passed(buffer, count, sem):
        part = buffer.at[0:count]
        pltpu.make_async_copy(part, part, sem).wait()

    for (dz, dy), copy in started:
        @pl.when(there[(dz, dy)])
        def _(copy=copy):
            copy.wait_send()
    to_partner.wait_send()

    @pl.when(is_early)
    def _():
        single[me] = counted
        passed(single, n_early - 1, one_send)
        passed(whole, (devices - n_early) // 2, all_send)
        passed(single, devices - 1, one_recv)
        totals_ref[...] = jnp.sum(single[...], axis=0)

    @pl.when(jnp.logical_not(is_early))
    def _():
        passed(single, n_early, one_send)
        passed(whole, (devices - n_early) // 2 - 1, all_send)
        passed(whole, devices // 2 - 1, all_recv)
        totals_ref[...] = jnp.sum(whole[...], axis=0)


def deliver(state, totals, state_out, totals_out, numbers, sems):
    whole_state = pltpu.make_async_copy(state, state_out, sems.at[0])
    whole_state.start()
    row = totals[...]
    lane = lax.broadcasted_iota(jnp.int32, row.shape, 1)
    for r in range(ROUNDS):
        numbers[r] = jnp.sum(jnp.where(lane == r, row, 0.0)).astype(jnp.int32)
    all_numbers = pltpu.make_async_copy(numbers, totals_out, sems.at[1])
    all_numbers.start()
    whole_state.wait()
    all_numbers.wait()


def per_device(nz, ny, ranks, seeds, flags):
    depth, rows, width = ranks.shape
    f32, i32, vmem, dma = jnp.float32, jnp.int32, pltpu.VMEM, pltpu.SemaphoreType.DMA
    plane = (rows, width)
    scratch = [
        vmem(ranks.shape, f32), vmem(seeds.shape, f32), vmem(flags.shape, i32),
        vmem(ranks.shape, i32), vmem((depth + 2, *plane), f32), vmem((depth + 2, *plane), f32), vmem(plane, f32),
        vmem((3, depth, 1, width), f32), vmem((3, depth, 1, width), f32),
        vmem((4, 1, width), f32), vmem((4, 1, width), f32),
        vmem((ROUNDS, depth + 2, *plane), f32), vmem((ROUNDS, depth, *plane), f32), vmem((ROUNDS, 2, *plane), f32),
        vmem((depth + 2, *plane), i32),
        vmem((ROUNDS, 2, 2, depth, 1, width), f32), vmem((ROUNDS, 2, 2, depth, 1, width), f32),
        vmem((ROUNDS, 4, 2, 1, width), f32), vmem((ROUNDS, 4, 2, 1, width), f32),
        vmem((2, 1, 128), f32), vmem((nz * ny, 1, 128), f32), vmem((nz * ny // 2, 1, 128), f32),
        pltpu.SemaphoreType.REGULAR((ROUNDS + 2,)), dma((3,)), dma((8,)), dma((8,)), dma((ROUNDS, 10)), dma((ROUNDS, 10)),
        dma, dma, dma, dma, dma, dma,
    ]
    state, totals = pl.pallas_call(
        functools.partial(kernel, nz, ny),
        out_shape=(vmem(ranks.shape, i32), vmem((1, 128), f32)),
        in_specs=[pl.BlockSpec(memory_space=pl.ANY)] * 3,
        out_specs=(pl.BlockSpec(memory_space=pltpu.VMEM), pl.BlockSpec(memory_space=pltpu.VMEM)),
        scratch_shapes=scratch,
        compiler_params=pltpu.CompilerParams(collective_id=0, has_side_effects=True),
    )(ranks, seeds, flags)
    return pl.pallas_call(
        deliver,
        out_shape=(jax.ShapeDtypeStruct(ranks.shape, i32), jax.ShapeDtypeStruct((ROUNDS,), i32)),
        in_specs=[pl.BlockSpec(memory_space=pltpu.VMEM)] * 2,
        out_specs=(pl.BlockSpec(memory_space=pl.ANY), pl.BlockSpec(memory_space=pl.ANY)),
        scratch_shapes=[pltpu.SMEM((ROUNDS,), i32), dma((2,))],
    )(*[pltpu.with_memory_space_constraint(x, pltpu.VMEM) for x in (state, totals)])


def solution(mesh):
    nz, ny = mesh.shape["gz"], mesh.shape["gy"]
    return jax.shard_map(
        functools.partial(per_device, nz, ny), mesh=mesh,
        in_specs=(P("gz", "gy", None), P(None, "gz", "gy", None), P("gz", "gy", None)),
        out_specs=(P("gz", "gy", None), P()), check_vma=False,
    )
```
